256 devices in a mesh: seq: 64 (over z_lo, x, y), tp: 4 (over z_hi, core).
Axes of the slice: x: 4, y: 4, z: 8 (z_hi: 2, z_lo: 4; z = z_hi * 4 + z_lo), core: 2. Of those that a mesh axis runs over, the one named last changes fastest.
Arguments:
- states: bfloat16 [64, 128, 2048], P('seq', None, 'tp'), may hold values from -60 to 60, as said below
- cotangent: bfloat16 [64, 128, 2048], P('seq', None, 'tp'), may hold values from -12 to 12, as said below
- wq: bfloat16 [2048, 2048], P(None, 'tp'), may hold values from -0.125 to 0.125
- wk: bfloat16 [2048, 512], P(None, 'tp'), may hold values from -0.125 to 0.125
- wv: bfloat16 [2048, 512], P(None, 'tp'), may hold values from -0.125 to 0.125
- wo: bfloat16 [2048, 2048], P('tp'), may hold values from -0.125 to 0.125
Outputs:
- gram: float32 [64, 64], P('seq')
The draws below stay inside these ranges and needn't reach their ends.
Inputs may be any that keep to these rules, and one draw needn't show every extreme that they name: `states`: finite values. `cotangent`: finite values.
All inputs are finite; a program needn't handle non-finite values.
Results may differ from the reference program's by a relative error of at most 0.0025.
Values may be sent and summed in bfloat16 or wider, within the bound.
No kernel may reach another device: no remote copies, remote signals or barrier semaphores. Data moves between devices by JAX's collectives and lax.ppermute only.
A program may use at most 64 MiB of HBM per device.

```python
import jax
import jax.numpy as jnp
from jax import lax

D = 2048
HEADS = 32
KV_HEADS = 8
HEAD_DIM = 64
TOKENS_PER_SEQ = 128
SEQUENCE_COUNT = 64


def candidate_rows(key):
    pick_key = jax.random.fold_in(key, 17)
    picked = jax.random.randint(pick_key, (SEQUENCE_COUNT, TOKENS_PER_SEQ), 0, 2).astype(jnp.int32)
    return picked + 2 * jnp.arange(TOKENS_PER_SEQ, dtype=jnp.int32)[None, :]


def draw_states(key, part):
    row_index = candidate_rows(key)
    table_key = jax.random.fold_in(key, 301)
    noise_key = jax.random.fold_in(key, 302)
    candidates = jax.random.normal(table_key, (2 * TOKENS_PER_SEQ, D), jnp.float32)
    noise = 0.4 * jax.random.normal(noise_key, (SEQUENCE_COUNT, TOKENS_PER_SEQ, D), jnp.float32)
    tokens_base = jnp.take(candidates, row_index, axis=0)
    return jnp.clip(tokens_base + noise, -12.0, 12.0).astype(jnp.bfloat16)


def draw_cotangent(key, part):
    row_index = candidate_rows(key)
    table_key = jax.random.fold_in(key, 401)
    noise_key = jax.random.fold_in(key, 402)
    candidates = jax.random.normal(table_key, (2 * TOKENS_PER_SEQ, D), jnp.float32)
    noise = 0.4 * jax.random.normal(noise_key, (SEQUENCE_COUNT, TOKENS_PER_SEQ, D), jnp.float32)
    tokens_base = jnp.take(candidates, row_index, axis=0)
    return jnp.clip(tokens_base + noise, -12.0, 12.0).astype(jnp.bfloat16)


def shard_levels(own_key, shape, cuts, low, high):
    def one(axis_at, parts):
        draws = jax.random.uniform(jax.random.fold_in(jax.random.fold_in(own_key, 6), axis_at), (parts,), jnp.float32, low / len(cuts), high / len(cuts))
        return jnp.repeat(jnp.exp(draws), shape[axis_at] // parts).reshape((-1,) + (1,) * (len(shape) - axis_at - 1))

    gain = one(*cuts[0])
    for cut in cuts[1:]:
        gain = gain * one(*cut)
    return gain


def centred(rng, extent, deviation, limit, shards=(), kind=jnp.bfloat16):
    drawn = deviation * jax.random.normal(rng, extent, jnp.float32)
    if shards:
        drawn = drawn * shard_levels(rng, extent, shards, -0.22, 0.18)
    return jnp.clip(drawn, -limit, limit).astype(kind)


def setup_inputs(seed: int = 0) -> dict:
    seeds = jax.random.split(jax.random.key(seed), 7)
    return {
        "states": draw_states(jax.random.fold_in(seeds[6], 71), 0),
        "cotangent": draw_cotangent(jax.random.fold_in(seeds[6], 71), 0),
        "wq": centred(seeds[2], (D, D), D ** -0.5, 0.125, ((1, 4),)),
        "wk": centred(seeds[3], (D, KV_HEADS * HEAD_DIM), D ** -0.5, 0.125, ((1, 4),)),
        "wv": centred(seeds[4], (D, KV_HEADS * HEAD_DIM), D ** -0.5, 0.125, ((1, 4),)),
        "wo": centred(seeds[5], (D, D), D ** -0.5, 0.125, ((0, 4),)),
    }


theta_base = 500000.0

def rope_tables(length, head_dim):
    half_dim = head_dim // 2
    freqs_k = theta_base ** (-(jnp.arange(half_dim, dtype=jnp.float32) * 2.0 / head_dim))
    angles = jnp.arange(length, dtype=jnp.float32)[:, None] * freqs_k[None, :]
    angles = jnp.concatenate([angles, angles], axis=1)
    return (jnp.cos(angles)[:, None, :], jnp.sin(angles)[:, None, :])

def rotate(values_in, cos_table, sine_table):
    half_dim = values_in.shape[-1] // 2
    turned = jnp.concatenate([-values_in[..., half_dim:], values_in[..., :half_dim]], axis=-1)
    return values_in * cos_table + turned * sine_table

def reference(states, cotangent, wq, wk, wv, wo):
    seqs, length, model_width = states.shape
    group_size = HEADS // KV_HEADS
    tok_rows = seqs * length
    cos_table, sine_table = rope_tables(length, HEAD_DIM)
    flat_states = states.reshape(tok_rows, model_width)
    query_heads = jnp.dot(flat_states, wq, preferred_element_type=jnp.float32).reshape(seqs, length, HEADS, HEAD_DIM)
    query_heads = rotate(query_heads, cos_table, sine_table).astype(jnp.bfloat16).reshape(seqs, length, KV_HEADS, group_size, HEAD_DIM)
    key_heads = jnp.dot(flat_states, wk, preferred_element_type=jnp.float32).reshape(seqs, length, KV_HEADS, HEAD_DIM)
    key_heads = rotate(key_heads, cos_table, sine_table).astype(jnp.bfloat16)
    value_heads = jnp.dot(flat_states, wv, preferred_element_type=jnp.float32).astype(jnp.bfloat16).reshape(seqs, length, KV_HEADS, HEAD_DIM)
    scores = jnp.einsum('sqkgd,stkd->skgqt', query_heads.astype(jnp.float32), key_heads.astype(jnp.float32)) * HEAD_DIM ** (-0.5)
    causal = jnp.arange(length)[:, None] >= jnp.arange(length)[None, :]
    scores = jnp.where(causal, scores, -jnp.inf)
    weights_bf = jax.nn.softmax(scores, axis=-1).astype(jnp.bfloat16)
    attended = jnp.einsum('skgqt,stkd->sqkgd', weights_bf.astype(jnp.float32), value_heads.astype(jnp.float32)).astype(jnp.bfloat16).reshape(seqs, length, model_width)
    grad_attended = lax.dot_general(cotangent.reshape(tok_rows, model_width), wo, (((1,), (1,)), ((), ())), preferred_element_type=jnp.float32).astype(jnp.bfloat16).reshape(seqs, length, KV_HEADS, group_size, HEAD_DIM)
    value_gradient = jnp.einsum('skgqt,sqkgd->stkd', weights_bf.astype(jnp.float32), grad_attended.astype(jnp.float32)).astype(jnp.bfloat16).reshape(seqs, length, KV_HEADS * HEAD_DIM)
    states_wide = states.astype(jnp.float32)
    grad_wv = jnp.einsum('std,stv->sdv', states_wide, value_gradient.astype(jnp.float32), precision=lax.Precision.HIGHEST)
    kernel = jnp.einsum('sdv,rdv->sr', grad_wv, grad_wv, precision=lax.Precision.HIGHEST)
    attended_wide = attended.astype(jnp.float32)
    cot_wide = cotangent.astype(jnp.float32)
    block_cols = model_width // 8

    def block_term(begin_col):
        cot_block = lax.dynamic_slice_in_dim(cot_wide, begin_col, block_cols, 2)
        grad_wo = jnp.einsum('std,ste->sde', attended_wide, cot_block, precision=lax.Precision.HIGHEST)
        return jnp.einsum('sde,rde->sr', grad_wo, grad_wo, precision=lax.Precision.HIGHEST)
    starts = (jnp.arange(8) * block_cols).astype(jnp.int32)
    kernel = kernel + lax.optimization_barrier(jnp.sum(lax.map(block_term, starts), axis=0))
    kernel_diag = jnp.diagonal(kernel)
    return kernel / jnp.sqrt(kernel_diag[:, None] * kernel_diag[None, :])
```

```python
import jax
import jax.numpy as jnp
from jax import lax
from jax.sharding import Mesh
from jax.sharding import PartitionSpec as P

HEADS = 32
KV_HEADS = 8
HEAD_DIM = 64
SEQ = ("zb", "za", "x", "y")
NEAR = ("za", "x", "y")
TP = ("h", "c")
EVERY = SEQ + TP
SWAP = ((0, 1), (1, 0))

theta_base = 500000.0


def swapped(value, axis):
    return lax.ppermute(value, axis, SWAP)


def in_order(own, other, axis, dim):
    first = lax.axis_index(axis) == 0
    return jnp.where(
        first,
        jnp.concatenate([own, other], axis=dim),
        jnp.concatenate([other, own], axis=dim),
    )


def all_features(part):
    far = swapped(part, "h")
    near = in_order(part, swapped(part, "c"), "c", 1)
    far = in_order(far, swapped(far, "c"), "c", 1)
    return in_order(near, far, "h", 1)


def rope_tables(length, head_dim):
    half_dim = head_dim // 2
    freqs_k = theta_base ** (-(jnp.arange(half_dim, dtype=jnp.float32) * 2.0 / head_dim))
    angles = jnp.arange(length, dtype=jnp.float32)[:, None] * freqs_k[None, :]
    angles = jnp.concatenate([angles, angles], axis=1)
    return (jnp.cos(angles)[:, None, :], jnp.sin(angles)[:, None, :])


def rotate(values_in, cos_table, sine_table):
    half_dim = values_in.shape[-1] // 2
    turned = jnp.concatenate([-values_in[..., half_dim:], values_in[..., :half_dim]], axis=-1)
    return values_in * cos_table + turned * sine_table


def attention_factors(full_states, full_cot, wq, wk, wv, wo):
    length = full_states.shape[0]
    kv_local = wk.shape[1] // HEAD_DIM
    group_size = HEADS // KV_HEADS
    cos_table, sine_table = rope_tables(length, HEAD_DIM)

    def project(w):
        return jnp.dot(full_states, w, preferred_element_type=jnp.float32)

    query_heads = project(wq).reshape(length, kv_local * group_size, HEAD_DIM)
    query_heads = (
        rotate(query_heads, cos_table, sine_table)
        .astype(jnp.bfloat16)
        .reshape(length, kv_local, group_size, HEAD_DIM)
    )
    key_heads = project(wk).reshape(length, kv_local, HEAD_DIM)
    key_heads = rotate(key_heads, cos_table, sine_table).astype(jnp.bfloat16)
    value_heads = project(wv).astype(jnp.bfloat16).reshape(length, kv_local, HEAD_DIM)
    scores = jnp.einsum(
        "qkgd,tkd->kgqt", query_heads, key_heads, preferred_element_type=jnp.float32
    ) * HEAD_DIM ** (-0.5)
    causal = jnp.arange(length)[:, None] >= jnp.arange(length)[None, :]
    scores = jnp.where(causal, scores, -jnp.inf)
    weights_bf = jax.nn.softmax(scores, axis=-1).astype(jnp.bfloat16)
    attended = (
        jnp.einsum("kgqt,tkd->qkgd", weights_bf, value_heads, preferred_element_type=jnp.float32)
        .astype(jnp.bfloat16)
        .reshape(length, -1)
    )
    grad_attended = (
        lax.dot_general(
            full_cot, wo, (((1,), (1,)), ((), ())), preferred_element_type=jnp.float32
        )
        .astype(jnp.bfloat16)
        .reshape(length, kv_local, group_size, HEAD_DIM)
    )
    value_gradient = (
        jnp.einsum("kgqt,qkgd->tkd", weights_bf, grad_attended, preferred_element_type=jnp.float32)
        .astype(jnp.bfloat16)
        .reshape(length, -1)
    )
    return jnp.concatenate([attended, value_gradient], axis=1)


def rows_by(left, right):
    return lax.dot_general(
        left, right, (((0,), (0,)), ((), ())), preferred_element_type=jnp.float32
    ).astype(jnp.bfloat16)


def gradient_blocks(factors, cot_half, states_half, blocks):
    part_width = HEADS * HEAD_DIM // 4
    both = jnp.concatenate(
        [
            rows_by(factors[:, :part_width], cot_half),
            rows_by(factors[:, part_width:], states_half),
        ],
        axis=0,
    )
    rows, cols = both.shape
    tall = blocks // (cols // 128)
    both = both.reshape(tall, rows // tall, cols // 128, 128)
    return jnp.transpose(both, (0, 2, 1, 3)).reshape(blocks, rows // tall, 128)


def on_device(states, cotangent, wq, wk, wv, wo):
    full_states = all_features(states[0])
    full_cot = all_features(cotangent[0])
    length, width = full_states.shape
    zb = lax.axis_index("zb")
    core = lax.axis_index("c")

    def sent_half(full):
        part = width // 4
        start = (1 - zb) * (2 * part) + core * part
        piece = lax.dynamic_slice_in_dim(full, start, part, 1)
        piece = swapped(piece, "zb")
        return in_order(piece, swapped(piece, "c"), "c", 1)

    def own_half(full):
        return jnp.where(zb == 0, full[:, : width // 2], full[:, width // 2 :])

    other_states, other_cot = sent_half(full_states), sent_half(full_cot)
    factors = attention_factors(full_states, full_cot, wq, wk, wv, wo)
    other_factors = swapped(factors, "zb")
    blocks = lax.axis_size(NEAR)
    own_blocks = gradient_blocks(factors, own_half(full_cot), own_half(full_states), blocks)
    other_blocks = gradient_blocks(other_factors, other_cot, other_states, blocks)
    sent = jnp.stack([own_blocks, other_blocks], axis=1)
    got = lax.all_to_all(sent, NEAR, 0, 0, tiled=True)
    seqs = 2 * blocks
    got = jnp.swapaxes(got, 0, 1).reshape(seqs, *got.shape[2:])
    share = jnp.einsum("irc,jrc->ij", got, got, preferred_element_type=jnp.float32)
    share = jnp.where(zb == 0, share, jnp.roll(share, (blocks, blocks), (0, 1)))
    rows = jnp.concatenate(
        [share, jnp.broadcast_to(jnp.diagonal(share)[None], share.shape)], axis=1
    )
    copies = lax.axis_size(TP)
    rows = jnp.broadcast_to(rows[:, None], (seqs, copies, 2 * seqs)).reshape(seqs * copies, 2 * seqs)
    total = jnp.sum(lax.all_to_all(rows, EVERY, 0, 0, tiled=True), axis=0, keepdims=True)
    row, diag = total[:, :seqs], total[:, seqs:]
    own_diag = lax.dynamic_slice_in_dim(diag, lax.axis_index(SEQ), 1, 1)
    return row / jnp.sqrt(own_diag * diag)


def solution(mesh):
    split = Mesh(
        mesh.devices.reshape(2, mesh.shape["seq"] // 32, 4, 4, 2, 2), EVERY
    )
    placed = (
        P(SEQ, None, TP),
        P(SEQ, None, TP),
        P(None, TP),
        P(None, TP),
        P(None, TP),
        P(TP, None),
    )
    return jax.shard_map(
        on_device, mesh=split, in_specs=placed, out_specs=P(SEQ, None), check_vma=False
    )
```

```python
import functools

import jax
import jax.numpy as jnp
from jax import lax
from jax.experimental import pallas as pl
from jax.experimental.pallas import tpu as pltpu
from jax.sharding import Mesh
from jax.sharding import PartitionSpec as P

HEADS = 32
KV_HEADS = 8
HEAD_DIM = 64
LANES = 128
SEQ = ("zb", "za", "x", "y")
NEAR = ("za", "x", "y")
TP = ("h", "c")
EVERY = SEQ + TP
SWAP = ((0, 1), (1, 0))

theta_base = 500000.0


def swapped(value, axis):
    return lax.ppermute(value, axis, SWAP)


def rope_tables(length, head_dim):
    half_dim = head_dim // 2
    freqs_k = theta_base ** (-(jnp.arange(half_dim, dtype=jnp.float32) * 2.0 / head_dim))
    angles = jnp.arange(length, dtype=jnp.float32)[:, None] * freqs_k[None, :]
    sine = jnp.sin(angles)
    cos = jnp.tile(jnp.cos(angles), (1, LANES // half_dim))
    return cos, jnp.tile(jnp.concatenate([-sine, sine], axis=1), (1, LANES // head_dim))


def dot(left, right, dims=((1,), (0,))):
    return lax.dot_general(left, right, (dims, ((), ())), preferred_element_type=jnp.float32)


def kernel_call(body, outs, ins, scratch=(), vmem_mib=24):
    smem = pl.BlockSpec(memory_space=pltpu.SMEM)
    vmem = pl.BlockSpec(memory_space=pltpu.VMEM)
    return pl.pallas_call(
        body,
        out_shape=outs,
        in_specs=[smem if a.dtype == jnp.int32 else vmem for a in ins],
        out_specs=jax.tree.map(lambda _: vmem, outs),
        scratch_shapes=scratch,
        compiler_params=pltpu.CompilerParams(vmem_limit_bytes=vmem_mib * 2**20),
    )(*ins)


def lower_half(shape):
    return lax.broadcasted_iota(jnp.int32, shape, 1) % (2 * HEAD_DIM) < HEAD_DIM


def doubled(pair, low):
    turned = pltpu.roll(pair, HEAD_DIM, 1)
    return jnp.where(low, pair, turned), jnp.where(low, turned, pair)


def attention_body(at, s0, s1, s2, s3, wq, wk, wv, cos_ref, sine_ref, attended, probs):
    quarter = s0.shape[1]
    h, c = at[0], at[1]
    places = [2 * h + c, 2 * h + 1 - c, 2 * (1 - h) + c, 2 * (1 - h) + 1 - c]
    parts = [s0[...], s1[...], s2[...], s3[...]]

    def project(w):
        total = None
        for part, place in zip(parts, places):
            rows = pl.ds(pl.multiple_of(place * quarter, quarter), quarter)
            term = dot(part, w[rows, :])
            total = term if total is None else total + term
        return total

    cos, sine = cos_ref[...], sine_ref[...]
    length = cos.shape[0]
    lane = lax.broadcasted_iota(jnp.int32, cos.shape, 1)
    first = lane % HEAD_DIM < HEAD_DIM // 2
    low = lower_half(cos.shape)

    def rotate(tile):
        ahead = pltpu.roll(tile, LANES - HEAD_DIM // 2, 1)
        behind = pltpu.roll(tile, HEAD_DIM // 2, 1)
        return tile * cos + jnp.where(first, ahead, behind) * sine

    keys = doubled(rotate(project(wk)), low)
    keys = [k.astype(jnp.bfloat16) for k in keys]
    values = [v.astype(jnp.bfloat16) for v in doubled(project(wv), low)]
    queries = project(wq)
    causal = lax.broadcasted_iota(jnp.int32, (length, length), 0) >= lax.broadcasted_iota(
        jnp.int32, (length, length), 1
    )
    tiles = queries.shape[1] // LANES
    for t in range(tiles):
        group = 2 * t // (HEADS // KV_HEADS)
        query = rotate(queries[:, t * LANES : (t + 1) * LANES])
        found = []
        for s in range(2):
            mine = low if s == 0 else jnp.logical_not(low)
            q = jnp.where(mine, query, 0.0).astype(jnp.bfloat16)
            scores = dot(q, keys[group], ((1,), (1,))) * HEAD_DIM ** (-0.5)
            scores = jnp.where(causal, scores, -jnp.inf)
            e = jnp.exp(scores - jnp.max(scores, axis=1, keepdims=True))
            p = (e / jnp.sum(e, axis=1, keepdims=True)).astype(jnp.bfloat16)
            probs[(2 * t + s) * length : (2 * t + s + 1) * length, :] = p
            found.append(dot(p, values[group]))
        tile = jnp.where(low, found[0], found[1])
        attended[:, t * LANES : (t + 1) * LANES] = tile.astype(jnp.bfloat16)


def put_blocks(blocks, turned, kind_rows, cols, col_at):
    tall = blocks.shape[1]
    begin, end = kind_rows
    wide = cols.shape[1] // LANES
    across = 8
    product = dot(turned, cols).astype(jnp.bfloat16)
    row = begin
    while row < end:
        block_row = row // tall
        stop = min(end, (block_row + 1) * tall)
        for j in range(wide):
            blocks[block_row * across + col_at + j, row - block_row * tall : stop - block_row * tall, :] = product[
                row - begin : stop - begin, j * LANES : (j + 1) * LANES
            ]
        row = stop


def grads_body(
    at, c0, c1, c2, c3, s0, s1, s2, s3, wo, attended, probs, factors, blocks
):
    quarter = c0.shape[1]
    length = c0.shape[0]
    h, c, zb = at[0], at[1], at[2]
    places = [2 * h + c, 2 * h + 1 - c, 2 * (1 - h) + c, 2 * (1 - h) + 1 - c]
    grads = None
    for part, place in zip((c0, c1, c2, c3), places):
        cols = pl.ds(pl.multiple_of(place * quarter, quarter), quarter)
        term = dot(part[...], wo[:, cols], ((1,), (1,)))
        grads = term if grads is None else grads + term
    low = lower_half((length, LANES))
    group_size = HEADS // KV_HEADS
    tiles = grads.shape[1] // LANES
    sums = []
    for g in range(2):
        stacked = []
        for t in range(g * group_size // 2, (g + 1) * group_size // 2):
            tile = grads[:, t * LANES : (t + 1) * LANES]
            stacked.append(jnp.where(low, tile, 0.0).astype(jnp.bfloat16))
            stacked.append(jnp.where(low, 0.0, tile).astype(jnp.bfloat16))
        rows = group_size * length
        found = dot(probs[g * rows : (g + 1) * rows, :], jnp.concatenate(stacked, 0), ((0,), (0,)))
        sums.append(found + pltpu.roll(found, HEAD_DIM, 1))
    value_gradient = jnp.where(low, sums[0], sums[1]).astype(jnp.bfloat16)
    width = attended.shape[1]
    factors[:, :width] = attended[...]
    factors[:, width:] = value_gradient
    here = h == zb
    turned_a = attended[...].T
    turned_v = value_gradient.T
    swap = c == 1
    for k, ((cn, cf), (sn, sf)) in enumerate((((c0, c2), (s0, s2)), ((c1, c3), (s1, s3)))):
        cot = jnp.where(here, cn[...], cf[...])
        state = jnp.where(here, sn[...], sf[...])
        col_at = jnp.where(swap, 1 - k, k) * (quarter // LANES)
        put_blocks(blocks, turned_a, (0, width), cot, col_at)
        put_blocks(blocks, turned_v, (width, width + LANES), state, col_at)


def other_body(at, c0, c1, s0, s1, factors, blocks):
    quarter = c0.shape[1]
    width = factors.shape[1] - LANES
    swap = at[1] == 1
    turned_a = factors[:, :width].T
    turned_v = factors[:, width:].T
    for k, (cot, state) in enumerate(((c0, s0), (c1, s1))):
        col_at = jnp.where(swap, 1 - k, k) * (quarter // LANES)
        put_blocks(blocks, turned_a, (0, width), cot[...], col_at)
        put_blocks(blocks, turned_v, (width, width + LANES), state[...], col_at)


def share_body(at, own, other, rows_out, wide):
    zb = at[2]
    seqs, tall, _ = own.shape
    for k, ref in enumerate((own, other)):
        base = jnp.where(zb == k, 0, seqs)
        for s in range(seqs):
            start = pl.multiple_of((base + s) * tall, 8)
            wide[pl.ds(start, tall), :] = ref[s].astype(jnp.float32)
    total = jnp.zeros((2 * seqs, 2 * seqs), jnp.float32)
    for r in range(0, tall, 2):
        pair = [
            wide[pl.ds(r + k, 2 * seqs, stride=tall), :].astype(jnp.bfloat16) for k in range(2)
        ]
        x = jnp.concatenate(pair, axis=1)
        total = total + dot(x, x, ((1,), (1,)))
    eye = lax.broadcasted_iota(jnp.int32, total.shape, 0) == lax.broadcasted_iota(
        jnp.int32, total.shape, 1
    )
    diag = jnp.sum(jnp.where(eye, total, 0.0), axis=0, keepdims=True)
    rows = jnp.concatenate([total, jnp.broadcast_to(diag, total.shape)], axis=1)
    copies = rows_out.shape[0] // rows.shape[0]
    for k in range(copies):
        rows_out[pl.ds(k, rows.shape[0], stride=copies), :] = rows


def final_body(at, got, out):
    seqs = out.shape[1]
    total = jnp.sum(got[...], axis=0, keepdims=True)
    lane = lax.broadcasted_iota(jnp.int32, total.shape, 1)
    own_diag = jnp.sum(jnp.where(lane == at[3] + seqs, total, 0.0), axis=1, keepdims=True)
    diag = pltpu.roll(total, seqs, 1)
    out[...] = (total / jnp.sqrt(own_diag * diag))[:, :seqs]


def on_device(states, cotangent, wq, wk, wv, wo):
    bf16, f32 = jnp.bfloat16, jnp.float32
    length, part = states.shape[1:]
    at = jnp.stack([lax.axis_index("h"), lax.axis_index("c"), lax.axis_index("zb"), lax.axis_index(SEQ)])
    at = at.astype(jnp.int32)
    zb_is_0 = lax.axis_index("zb") == 0
    h_is_0 = lax.axis_index("h") == 0

    def gathered(own):
        far = swapped(own, "h")
        return own, swapped(own, "c"), far, swapped(far, "c")

    s = gathered(states[0])
    k = gathered(cotangent[0])
    cos, sine = rope_tables(length, HEAD_DIM)
    attended, probs = kernel_call(
        attention_body,
        (
            jax.ShapeDtypeStruct((length, part), bf16),
            jax.ShapeDtypeStruct((part // HEAD_DIM * length, length), bf16),
        ),
        (at, *s, wq, wk, wv, cos, sine),
    )
    blocks = lax.axis_size(NEAR)
    tall = (part + LANES) * (2 * part) // (LANES * blocks)
    block_shape = jax.ShapeDtypeStruct((blocks, tall, LANES), bf16)
    factors, own_blocks = kernel_call(
        grads_body,
        (jax.ShapeDtypeStruct((length, part + LANES), bf16), block_shape),
        (at, *k, *s, wo, attended, probs),
    )
    got_own = lax.all_to_all(own_blocks, NEAR, 0, 0, tiled=True)

    def partner(parts):
        own, _, far, _ = parts
        piece = swapped(jnp.where(h_is_0 == zb_is_0, far, own), "zb")
        return piece, swapped(piece, "c")

    other_factors = swapped(factors, "zb")
    other_blocks = kernel_call(
        other_body, block_shape, (at, *partner(k), *partner(s), other_factors)
    )
    got_other = lax.all_to_all(other_blocks, NEAR, 0, 0, tiled=True)
    seqs = 2 * blocks
    copies = lax.axis_size(TP)
    rows = kernel_call(
        share_body,
        jax.ShapeDtypeStruct((seqs * copies, 2 * seqs), f32),
        (at, got_own, got_other),
        (pltpu.VMEM((seqs * tall, LANES), f32),),
    )
    rows = rows.reshape(seqs * copies, 1, 2 * seqs)
    got = lax.all_to_all(rows, EVERY, 0, 0, tiled=True).reshape(seqs * copies, 2 * seqs)
    return kernel_call(final_body, jax.ShapeDtypeStruct((1, seqs), f32), (at, got))


def solution(mesh):
    split = Mesh(mesh.devices.reshape(2, mesh.shape["seq"] // 32, 4, 4, 2, 2), EVERY)
    placed = (
        P(SEQ, None, TP),
        P(SEQ, None, TP),
        P(None, TP),
        P(None, TP),
        P(None, TP),
        P(TP, None),
    )
    return jax.shard_map(
        on_device, mesh=split, in_specs=placed, out_specs=P(SEQ, None), check_vma=False
    )
```

```python
import jax
import jax.numpy as jnp
from jax import lax
from jax.experimental import pallas as pl
from jax.experimental.pallas import tpu as pltpu
from jax.sharding import Mesh
from jax.sharding import PartitionSpec as P


HEADS = 32
KV_HEADS = 8
HEAD_DIM = 64
LANES = 128
SEQ = ("zb", "za", "x", "y")
NEAR = ("za", "x", "y")
TP = ("h", "c")
EVERY = SEQ + TP
SWAP = ((0, 1), (1, 0))

theta_base = 500000.0


def swapped(value, axis):
    return lax.ppermute(value, axis, SWAP)


def rope_tables(length, head_dim):
    half_dim = head_dim // 2
    freqs_k = theta_base ** (-(jnp.arange(half_dim, dtype=jnp.float32) * 2.0 / head_dim))
    angles = jnp.arange(length, dtype=jnp.float32)[:, None] * freqs_k[None, :]
    sine = jnp.sin(angles)
    cos = jnp.tile(jnp.cos(angles), (1, LANES // half_dim))
    return cos, jnp.tile(jnp.concatenate([-sine, sine], axis=1), (1, LANES // head_dim))


def dot(left, right, dims=((1,), (0,))):
    return lax.dot_general(left, right, (dims, ((), ())), preferred_element_type=jnp.float32)


def kernel_call(body, outs, ins, scratch=(), vmem_mib=16, far=()):
    hbm = pl.BlockSpec(memory_space=pl.ANY)
    smem = pl.BlockSpec(memory_space=pltpu.SMEM)
    vmem = pl.BlockSpec(memory_space=pltpu.VMEM)
    return pl.pallas_call(
        body,
        out_shape=outs,
        in_specs=[
            hbm if i in far else smem if a.dtype == jnp.int32 else vmem for i, a in enumerate(ins)
        ],
        out_specs=jax.tree.map(lambda _: vmem, outs),
        scratch_shapes=scratch,
        compiler_params=pltpu.CompilerParams(vmem_limit_bytes=vmem_mib * 2**20),
    )(*ins)


def lower_half(shape):
    return lax.broadcasted_iota(jnp.int32, shape, 1) % (2 * HEAD_DIM) < HEAD_DIM


def doubled(pair, low):
    turned = pltpu.roll(pair, HEAD_DIM, 1)
    return jnp.where(low, pair, turned), jnp.where(low, turned, pair)


def places_of(at):
    h, c = at[0], at[1]
    return [2 * h + c, 2 * h + 1 - c, 2 * (1 - h) + c, 2 * (1 - h) + 1 - c]


def rows_at(place, size):
    return pl.ds(pl.multiple_of(place * size, size), size)


def start_body(
    at, s0, s1, c0, c1, wq, wk, wv, wo, s_out, c_out, wq_out, wk_out, wv_out, wo_out, sums, grads, sems
):
    moves = [
        pltpu.make_async_copy(src, dst, sems.at[i])
        for i, (src, dst) in enumerate(
            ((wq, wq_out), (wk, wk_out), (wv, wv_out), (wo, wo_out), (s0, s_out), (c0, c_out))
        )
    ]
    for move in moves:
        move.start()
    for move in moves:
        move.wait()
    quarter = s_out.shape[1]
    near = places_of(at)[:2]
    begin = 0
    for w in (wq_out, wk_out, wv_out):
        end = begin + w.shape[1]
        sums[:, begin:end] = dot(s_out[...], w[rows_at(near[0], quarter), :]) + dot(
            s1[...], w[rows_at(near[1], quarter), :]
        )
        begin = end
    nt = ((1,), (1,))
    grads[...] = dot(c_out[...], wo_out[:, rows_at(near[0], quarter)], nt) + dot(
        c1[...], wo_out[:, rows_at(near[1], quarter)], nt
    )


def attention_body(at, s2, s3, wq, wk, wv, sums, cos_ref, sine_ref, attended, probs):
    quarter = s2.shape[1]
    far = places_of(at)[2:]

    def project(w, begin):
        total = sums[:, begin : begin + w.shape[1]]
        for part, place in zip((s2, s3), far):
            total = total + dot(part[...], w[rows_at(place, quarter), :])
        return total

    cos, sine = cos_ref[...], sine_ref[...]
    length = cos.shape[0]
    lane = lax.broadcasted_iota(jnp.int32, cos.shape, 1)
    first = lane % HEAD_DIM < HEAD_DIM // 2
    low = lower_half(cos.shape)

    def rotate(tile):
        ahead = pltpu.roll(tile, LANES - HEAD_DIM // 2, 1)
        behind = pltpu.roll(tile, HEAD_DIM // 2, 1)
        return tile * cos + jnp.where(first, ahead, behind) * sine

    width = wq.shape[1]
    keys = [k.astype(jnp.bfloat16) for k in doubled(rotate(project(wk, width)), low)]
    values = [v.astype(jnp.bfloat16) for v in doubled(project(wv, width + LANES), low)]
    queries = project(wq, 0)
    causal = lax.broadcasted_iota(jnp.int32, (length, length), 0) >= lax.broadcasted_iota(
        jnp.int32, (length, length), 1
    )
    for t in range(width // LANES):
        group = 2 * t // (HEADS // KV_HEADS)
        query = rotate(queries[:, t * LANES : (t + 1) * LANES])
        found = []
        for s in range(2):
            mine = low if s == 0 else jnp.logical_not(low)
            q = jnp.where(mine, query, 0.0).astype(jnp.bfloat16)
            scores = dot(q, keys[group], ((1,), (1,))) * HEAD_DIM ** (-0.5)
            scores = jnp.where(causal, scores, -jnp.inf)
            e = jnp.exp(scores - jnp.max(scores, axis=1, keepdims=True))
            p = (e / jnp.sum(e, axis=1, keepdims=True)).astype(jnp.bfloat16)
            probs[(2 * t + s) * length : (2 * t + s + 1) * length, :] = p
            found.append(dot(p, values[group]))
        tile = jnp.where(low, found[0], found[1])
        attended[:, t * LANES : (t + 1) * LANES] = tile.astype(jnp.bfloat16)


def put_blocks(blocks, turned, kind_rows, cols, col_at):
    tall = blocks.shape[1]
    begin, end = kind_rows
    wide = cols.shape[1] // LANES
    across = 8
    product = dot(turned, cols).astype(jnp.bfloat16)
    row = begin
    while row < end:
        block_row = row // tall
        stop = min(end, (block_row + 1) * tall)
        for j in range(wide):
            blocks[block_row * across + col_at + j, row - block_row * tall : stop - block_row * tall, :] = product[
                row - begin : stop - begin, j * LANES : (j + 1) * LANES
            ]
        row = stop


def grads_body(at, c2, c3, wo, partial, attended, probs, factors):
    length, quarter = c2.shape
    grads = partial[...]
    for part, place in zip((c2, c3), places_of(at)[2:]):
        grads = grads + dot(part[...], wo[:, rows_at(place, quarter)], ((1,), (1,)))
    low = lower_half((length, LANES))
    group_size = HEADS // KV_HEADS
    sums = []
    for g in range(2):
        stacked = []
        for t in range(g * group_size // 2, (g + 1) * group_size // 2):
            tile = grads[:, t * LANES : (t + 1) * LANES]
            stacked.append(jnp.where(low, tile, 0.0).astype(jnp.bfloat16))
            stacked.append(jnp.where(low, 0.0, tile).astype(jnp.bfloat16))
        rows = group_size * length
        found = dot(probs[g * rows : (g + 1) * rows, :], jnp.concatenate(stacked, 0), ((0,), (0,)))
        sums.append(found + pltpu.roll(found, HEAD_DIM, 1))
    width = attended.shape[1]
    factors[:, :width] = attended[...]
    factors[:, width:] = jnp.where(low, sums[0], sums[1]).astype(jnp.bfloat16)


def put_all(at, factors, cots, states, blocks):
    width = factors.shape[1] - LANES
    turned_a = factors[:, :width].T
    turned_v = factors[:, width:].T
    for k, (cot, state) in enumerate(zip(cots, states)):
        col_at = jnp.where(at[1] == 1, 1 - k, k) * (cot.shape[1] // LANES)
        put_blocks(blocks, turned_a, (0, width), cot, col_at)
        put_blocks(blocks, turned_v, (width, width + LANES), state, col_at)


def own_body(at, c0, c1, c2, c3, s0, s1, s2, s3, factors, blocks):
    here = at[0] == at[2]

    def half(parts):
        return [jnp.where(here, parts[k][...], parts[k + 2][...]) for k in range(2)]

    put_all(at, factors, half((c0, c1, c2, c3)), half((s0, s1, s2, s3)), blocks)


def other_body(at, c0, c1, s0, s1, factors, blocks):
    put_all(at, factors, (c0[...], c1[...]), (s0[...], s1[...]), blocks)


def turn_blocks(got, wide, keep):
    seqs, tall, _ = got.shape
    for s in range(seqs):
        wide[pl.ds(s * tall, tall), :] = got[s].astype(jnp.float32)
    for r in range(tall):
        keep(r, wide[pl.ds(r, seqs, stride=tall), :].astype(jnp.bfloat16))


def turn_body(got, turned, wide):
    def keep(r, rows):
        turned[r] = rows

    turn_blocks(got, wide, keep)


def share_body(at, own, other, rows_out, wide):
    _, seqs, _ = own.shape
    straight = at[2] == 0
    total = jnp.zeros((2 * seqs, 2 * seqs), jnp.float32)
    waiting = []

    def keep(r, rows):
        nonlocal total
        mine = own[r]
        waiting.append(
            jnp.concatenate([jnp.where(straight, mine, rows), jnp.where(straight, rows, mine)], axis=0)
        )
        if len(waiting) == 2:
            x = jnp.concatenate(waiting, axis=1)
            total = total + dot(x, x, ((1,), (1,)))
            waiting.clear()

    turn_blocks(other, wide, keep)
    eye = lax.broadcasted_iota(jnp.int32, total.shape, 0) == lax.broadcasted_iota(
        jnp.int32, total.shape, 1
    )
    diag = jnp.sum(jnp.where(eye, total, 0.0), axis=0, keepdims=True)
    rows = jnp.concatenate([total, jnp.broadcast_to(diag, total.shape)], axis=1)
    copies = rows_out.shape[0] // rows.shape[0]
    for k in range(copies):
        rows_out[pl.ds(k, rows.shape[0], stride=copies), :] = rows


def final_body(at, got, out):
    seqs = out.shape[1]
    total = jnp.sum(got[...], axis=0, keepdims=True)
    lane = lax.broadcasted_iota(jnp.int32, total.shape, 1)
    own_diag = jnp.sum(jnp.where(lane == at[3] + seqs, total, 0.0), axis=1, keepdims=True)
    diag = pltpu.roll(total, seqs, 1)
    out[...] = (total / jnp.sqrt(own_diag * diag))[:, :seqs]


def on_device(states, cotangent, wq, wk, wv, wo):
    bf16, f32 = jnp.bfloat16, jnp.float32
    shape = jax.ShapeDtypeStruct
    length, part = states.shape[1:]
    states, cotangent = states[0], cotangent[0]
    axes = (lax.axis_index("h"), lax.axis_index("c"), lax.axis_index("zb"), lax.axis_index(SEQ))
    at = jnp.stack(axes).astype(jnp.int32)
    far_half = axes[0] == axes[2]
    blocks = lax.axis_size(NEAR)
    seqs = 2 * blocks
    tall = (part + LANES) * (2 * part) // (LANES * blocks)
    block_shape = shape((blocks, tall, LANES), bf16)
    wide = pltpu.VMEM((blocks * tall, LANES), f32)

    def gathered(own):
        far = swapped(own, "h")
        near = swapped(own, "c")
        return near, far, swapped(far, "c")

    def partner(own, far):
        piece = swapped(jnp.where(far_half, far, own), "zb")
        return piece, swapped(piece, "c")

    s1, s2, s3 = gathered(states)
    c1, c2, c3 = gathered(cotangent)
    cos, sine = rope_tables(length, HEAD_DIM)
    kv = wk.shape[1]
    s0, c0, wq, wk, wv, wo, sums, grads = kernel_call(
        start_body,
        (
            *(shape(a.shape, bf16) for a in (states, cotangent, wq, wk, wv, wo)),
            shape((length, part + 2 * kv), f32),
            shape((length, part), f32),
        ),
        (at, states, s1, cotangent, c1, wq, wk, wv, wo),
        (pltpu.SemaphoreType.DMA((6,)),),
        far=(1, 3, 5, 6, 7, 8),
    )
    attended, probs = kernel_call(
        attention_body,
        (shape((length, part), bf16), shape((part // HEAD_DIM * length, length), bf16)),
        (at, s2, s3, wq, wk, wv, sums, cos, sine),
    )
    factors = kernel_call(
        grads_body, shape((length, part + LANES), bf16), (at, c2, c3, wo, grads, attended, probs)
    )
    other_factors = swapped(factors, "zb")
    own_blocks = kernel_call(own_body, block_shape, (at, c0, c1, c2, c3, s0, s1, s2, s3, factors))
    got_own = lax.all_to_all(own_blocks, NEAR, 0, 0, tiled=True)
    other_blocks = kernel_call(
        other_body,
        block_shape,
        (at, *partner(c0, c2), *partner(s0, s2), other_factors),
    )
    got_other = lax.all_to_all(other_blocks, NEAR, 0, 0, tiled=True)
    own_turned = kernel_call(turn_body, shape((tall, blocks, LANES), bf16), (got_own,), (wide,))
    copies = lax.axis_size(TP)
    rows = kernel_call(
        share_body,
        shape((seqs * copies, 2 * seqs), f32),
        (at, own_turned, got_other),
        (wide,),
    )
    rows = rows.reshape(seqs * copies, 1, 2 * seqs)
    got = lax.all_to_all(rows, EVERY, 0, 0, tiled=True).reshape(seqs * copies, 2 * seqs)
    return kernel_call(final_body, shape((1, seqs), f32), (at, got))


def solution(mesh):
    split = Mesh(mesh.devices.reshape(2, mesh.shape["seq"] // 32, 4, 4, 2, 2), EVERY)
    placed = (
        P(SEQ, None, TP),
        P(SEQ, None, TP),
        P(None, TP),
        P(None, TP),
        P(None, TP),
        P(TP, None),
    )

    return jax.shard_map(
        on_device, mesh=split, in_specs=placed, out_specs=P(SEQ, None), check_vma=False
    )
```

```python
import jax
import jax.numpy as jnp
import numpy as np
from jax import lax
from jax.experimental import pallas as pl
from jax.experimental.pallas import tpu as pltpu
from jax.sharding import Mesh
from jax.sharding import PartitionSpec as P


HEADS = 32
KV_HEADS = 8
HEAD_DIM = 64
LANES = 128
SEQ = ("zb", "za", "x", "y")
NEAR = ("za", "x", "y")
TP = ("h", "c")
EVERY = SEQ + TP
SWAP = ((0, 1), (1, 0))

theta_base = 500000.0


def swapped(value, axis):
    return lax.ppermute(value, axis, SWAP)


def rope_tables(length, head_dim):
    half_dim = head_dim // 2
    steps = np.arange(half_dim, dtype=np.float32) * np.float32(2.0) / np.float32(head_dim)
    freqs_k = np.power(np.float32(theta_base), -steps)
    angles = np.arange(length, dtype=np.float32)[:, None] * freqs_k[None, :]
    sine = np.sin(angles)
    cos = np.tile(np.cos(angles), (1, LANES // half_dim))
    return cos, np.tile(np.concatenate([-sine, sine], axis=1), (1, LANES // head_dim))


def dot(left, right, dims=((1,), (0,))):
    return lax.dot_general(left, right, (dims, ((), ())), preferred_element_type=jnp.float32)


def kernel_call(body, outs, ins, scratch=(), vmem_mib=16, far=()):
    ins = [pltpu.with_memory_space_constraint(a, pltpu.HBM) if i in far else a for i, a in enumerate(ins)]
    hbm = pl.BlockSpec(memory_space=pltpu.HBM)
    smem = pl.BlockSpec(memory_space=pltpu.SMEM)
    vmem = pl.BlockSpec(memory_space=pltpu.VMEM)
    return pl.pallas_call(
        body,
        out_shape=outs,
        in_specs=[
            hbm if i in far else smem if a.dtype == jnp.int32 else vmem for i, a in enumerate(ins)
        ],
        out_specs=jax.tree.map(lambda _: vmem, outs),
        scratch_shapes=scratch,
        compiler_params=pltpu.CompilerParams(vmem_limit_bytes=vmem_mib * 2**20),
    )(*ins)


def lower_half(shape):
    return lax.broadcasted_iota(jnp.int32, shape, 1) % (2 * HEAD_DIM) < HEAD_DIM


def doubled(pair, low):
    turned = pltpu.roll(pair, HEAD_DIM, 1)
    return jnp.where(low, pair, turned), jnp.where(low, turned, pair)


def places_of(at):
    h, c = at[0], at[1]
    return [2 * h + c, 2 * h + 1 - c, 2 * (1 - h) + c, 2 * (1 - h) + 1 - c]


def rows_at(place, size):
    return pl.ds(pl.multiple_of(place * size, size), size)


def start_body(
    at, s0, s1, c0, c1, wq, wk, wv, wo, own, wq_out, wk_out, wv_out, wo_out, sums, grads, sems
):
    length = s0.shape[0]
    s_out, c_out = own.at[:length, :], own.at[length:, :]
    moves = [
        pltpu.make_async_copy(src, dst, sems.at[i])
        for i, (src, dst) in enumerate(
            ((wq, wq_out), (wk, wk_out), (wv, wv_out), (wo, wo_out), (s0, s_out), (c0, c_out))
        )
    ]
    for move in moves:
        move.start()
    for move in moves:
        move.wait()
    quarter = s_out.shape[1]
    near = places_of(at)[:2]
    begin = 0
    for w in (wq_out, wk_out, wv_out):
        end = begin + w.shape[1]
        sums[:, begin:end] = dot(s_out[...], w[rows_at(near[0], quarter), :]) + dot(
            s1[...], w[rows_at(near[1], quarter), :]
        )
        begin = end
    nt = ((1,), (1,))
    grads[...] = dot(c_out[...], wo_out[:, rows_at(near[0], quarter)], nt) + dot(
        c1[...], wo_out[:, rows_at(near[1], quarter)], nt
    )


def attention_body(at, s2, s3, wq, wk, wv, sums, cos_ref, sine_ref, attended, probs):
    quarter = s2.shape[1]
    far = places_of(at)[2:]

    def project(w, begin):
        total = sums[:, begin : begin + w.shape[1]]
        for part, place in zip((s2, s3), far):
            total = total + dot(part[...], w[rows_at(place, quarter), :])
        return total

    cos, sine = cos_ref[...], sine_ref[...]
    length = cos.shape[0]
    lane = lax.broadcasted_iota(jnp.int32, cos.shape, 1)
    first = lane % HEAD_DIM < HEAD_DIM // 2
    low = lower_half(cos.shape)

    def rotate(tile):
        ahead = pltpu.roll(tile, LANES - HEAD_DIM // 2, 1)
        behind = pltpu.roll(tile, HEAD_DIM // 2, 1)
        return tile * cos + jnp.where(first, ahead, behind) * sine

    width = wq.shape[1]
    keys = [k.astype(jnp.bfloat16) for k in doubled(rotate(project(wk, width)), low)]
    values = [v.astype(jnp.bfloat16) for v in doubled(project(wv, width + LANES), low)]
    queries = project(wq, 0)
    causal = lax.broadcasted_iota(jnp.int32, (length, length), 0) >= lax.broadcasted_iota(
        jnp.int32, (length, length), 1
    )
    for t in range(width // LANES):
        group = 2 * t // (HEADS // KV_HEADS)
        query = rotate(queries[:, t * LANES : (t + 1) * LANES])
        found = []
        for s in range(2):
            mine = low if s == 0 else jnp.logical_not(low)
            q = jnp.where(mine, query, 0.0).astype(jnp.bfloat16)
            scores = dot(q, keys[group], ((1,), (1,))) * HEAD_DIM ** (-0.5)
            scores = jnp.where(causal, scores, -jnp.inf)
            e = jnp.exp(scores - jnp.max(scores, axis=1, keepdims=True))
            p = (e / jnp.sum(e, axis=1, keepdims=True)).astype(jnp.bfloat16)
            probs[(2 * t + s) * length : (2 * t + s + 1) * length, :] = p
            found.append(dot(p, values[group]))
        tile = jnp.where(low, found[0], found[1])
        attended[:, t * LANES : (t + 1) * LANES] = tile.astype(jnp.bfloat16)


def put_blocks(blocks, turned, kind_rows, cols, col_at):
    tall = blocks.shape[1]
    begin, end = kind_rows
    wide = cols.shape[1] // LANES
    across = 8
    product = dot(turned, cols).astype(jnp.bfloat16)
    row = begin
    while row < end:
        block_row = row // tall
        stop = min(end, (block_row + 1) * tall)
        for j in range(wide):
            blocks[block_row * across + col_at + j, row - block_row * tall : stop - block_row * tall, :] = product[
                row - begin : stop - begin, j * LANES : (j + 1) * LANES
            ]
        row = stop


def grads_body(at, c2, c3, wo, partial, attended, probs, factors):
    length, quarter = c2.shape
    grads = partial[...]
    for part, place in zip((c2, c3), places_of(at)[2:]):
        grads = grads + dot(part[...], wo[:, rows_at(place, quarter)], ((1,), (1,)))
    low = lower_half((length, LANES))
    group_size = HEADS // KV_HEADS
    sums = []
    for g in range(2):
        stacked = []
        for t in range(g * group_size // 2, (g + 1) * group_size // 2):
            tile = grads[:, t * LANES : (t + 1) * LANES]
            stacked.append(jnp.where(low, tile, 0.0).astype(jnp.bfloat16))
            stacked.append(jnp.where(low, 0.0, tile).astype(jnp.bfloat16))
        rows = group_size * length
        found = dot(probs[g * rows : (g + 1) * rows, :], jnp.concatenate(stacked, 0), ((0,), (0,)))
        sums.append(found + pltpu.roll(found, HEAD_DIM, 1))
    width = attended.shape[1]
    factors[:, :width] = attended[...]
    factors[:, width:] = jnp.where(low, sums[0], sums[1]).astype(jnp.bfloat16)


def put_all(at, factors, cots, states, blocks):
    width = factors.shape[1] - LANES
    turned_a = factors[:, :width].T
    turned_v = factors[:, width:].T
    for k, (cot, state) in enumerate(zip(cots, states)):
        col_at = jnp.where(at[1] == 1, 1 - k, k) * (cot.shape[1] // LANES)
        put_blocks(blocks, turned_a, (0, width), cot, col_at)
        put_blocks(blocks, turned_v, (width, width + LANES), state, col_at)


def own_body(at, own, s1, s2, s3, c1, c2, c3, factors, blocks):
    here = at[0] == at[2]
    length = s1.shape[0]

    def half(p0, p1, p2, p3):
        return [jnp.where(here, p0, p2[...]), jnp.where(here, p1[...], p3[...])]

    states = half(own[:length, :], s1, s2, s3)
    cots = half(own[length:, :], c1, c2, c3)
    put_all(at, factors, cots, states, blocks)


def pick_body(at, same, cross, piece):
    piece[...] = jnp.where(at[0] == at[2], same[...], cross[...])


def other_body(at, piece, near, factors, blocks):
    length = factors.shape[0]
    states = [p[:length, :] for p in (piece, near)]
    cots = [p[length:, :] for p in (piece, near)]
    put_all(at, factors, cots, states, blocks)


def turn_blocks(got, wide, keep, ready=lambda: None):
    seqs, tall, _ = got.shape
    for s in range(seqs):
        wide[pl.ds(s * tall, tall), :] = got[s].astype(jnp.float32)
    ready()
    for r in range(tall):
        keep(r, wide[pl.ds(r, seqs, stride=tall), :].astype(jnp.bfloat16))


def turn_body(got, turned, wide):
    def keep(r, rows):
        turned[r] = rows

    turn_blocks(got, wide, keep)


def share_body(at, own_far, other, rows_out, wide, own, sem):
    _, seqs, _ = own.shape
    fetch = pltpu.make_async_copy(own_far, own, sem)
    fetch.start()
    straight = at[2] == 0
    total = jnp.zeros((2 * seqs, 2 * seqs), jnp.float32)
    waiting = []

    def keep(r, rows):
        nonlocal total
        mine = own[r]
        waiting.append(
            jnp.concatenate([jnp.where(straight, mine, rows), jnp.where(straight, rows, mine)], axis=0)
        )
        if len(waiting) == 2:
            x = jnp.concatenate(waiting, axis=1)
            total = total + dot(x, x, ((1,), (1,)))
            waiting.clear()

    turn_blocks(other, wide, keep, fetch.wait)
    eye = lax.broadcasted_iota(jnp.int32, total.shape, 0) == lax.broadcasted_iota(
        jnp.int32, total.shape, 1
    )
    diag = jnp.sum(jnp.where(eye, total, 0.0), axis=0, keepdims=True)
    rows = jnp.concatenate([total, jnp.broadcast_to(diag, total.shape)], axis=1)
    copies = rows_out.shape[0] // rows.shape[0]
    for k in range(copies):
        rows_out[pl.ds(k, rows.shape[0], stride=copies), :] = rows


def between_body(at, out):
    for k in range(at.shape[0]):
        out[k] = at[k]


def final_body(at, got, out):
    seqs = out.shape[1]
    total = jnp.sum(got[...], axis=0, keepdims=True)
    lane = lax.broadcasted_iota(jnp.int32, total.shape, 1)
    own_diag = jnp.sum(jnp.where(lane == at[3] + seqs, total, 0.0), axis=1, keepdims=True)
    diag = pltpu.roll(total, seqs, 1)
    out[...] = (total / jnp.sqrt(own_diag * diag))[:, :seqs]


def on_device(states, cotangent, wq, wk, wv, wo):
    bf16, f32 = jnp.bfloat16, jnp.float32
    shape = jax.ShapeDtypeStruct
    length, part = states.shape[1:]
    states, cotangent = states[0], cotangent[0]
    axes = (lax.axis_index("h"), lax.axis_index("c"), lax.axis_index("zb"), lax.axis_index(SEQ))
    at = jnp.stack(axes).astype(jnp.int32)
    blocks = lax.axis_size(NEAR)
    seqs = 2 * blocks
    tall = (part + LANES) * (2 * part) // (LANES * blocks)
    block_shape = shape((blocks, tall, LANES), bf16)
    wide = pltpu.VMEM((blocks * tall, LANES), f32)

    def gathered(own):
        far = swapped(own, "h")
        near = swapped(own, "c")
        return near, far, swapped(far, "c")

    s1, s2, s3 = gathered(states)
    c1, c2, c3 = gathered(cotangent)
    cos, sine = rope_tables(length, HEAD_DIM)
    kv = wk.shape[1]
    own, wq, wk, wv, wo, sums, grads = kernel_call(
        start_body,
        (
            shape((2 * length, part), bf16),
            *(shape(a.shape, bf16) for a in (wq, wk, wv, wo)),
            shape((length, part + 2 * kv), f32),
            shape((length, part), f32),
        ),
        (at, states, s1, cotangent, c1, wq, wk, wv, wo),
        (pltpu.SemaphoreType.DMA((6,)),),
        far=(1, 3, 5, 6, 7, 8),
    )
    same = lax.ppermute(own, ("zb", "h"), ((2, 0), (1, 3)))
    cross = lax.ppermute(own, ("zb", "h"), ((2, 1), (1, 2)))
    smem = pl.BlockSpec(memory_space=pltpu.SMEM)
    at_later = pl.pallas_call(
        between_body,
        out_shape=shape(at.shape, at.dtype),
        in_specs=[smem],
        out_specs=smem,
        compiler_params=pltpu.CompilerParams(vmem_limit_bytes=2**20),
    )(at)
    attended, probs = kernel_call(
        attention_body,
        (shape((length, part), bf16), shape((part // HEAD_DIM * length, length), bf16)),
        (at_later, s2, s3, wq, wk, wv, sums, cos, sine),
    )
    factors = kernel_call(
        grads_body, shape((length, part + LANES), bf16), (at, c2, c3, wo, grads, attended, probs)
    )
    other_factors = swapped(factors, "zb")
    own_blocks = kernel_call(own_body, block_shape, (at, own, s1, s2, s3, c1, c2, c3, factors))
    got_own = lax.all_to_all(own_blocks, NEAR, 0, 0, tiled=True)
    piece = kernel_call(pick_body, shape(own.shape, bf16), (at, same, cross))
    near = swapped(piece, "c")
    other_blocks = kernel_call(other_body, block_shape, (at, piece, near, other_factors))
    got_other = lax.all_to_all(other_blocks, NEAR, 0, 0, tiled=True)
    own_turned = kernel_call(turn_body, shape((tall, blocks, LANES), bf16), (got_own,), (wide,))
    copies = lax.axis_size(TP)
    rows = kernel_call(
        share_body,
        shape((seqs * copies, 2 * seqs), f32),
        (at, own_turned, got_other),
        (wide, pltpu.VMEM(own_turned.shape, bf16), pltpu.SemaphoreType.DMA),
        far=(1,),
    )
    rows = rows.reshape(seqs * copies, 1, 2 * seqs)
    got = lax.all_to_all(rows, EVERY, 0, 0, tiled=True).reshape(seqs * copies, 2 * seqs)
    return kernel_call(final_body, shape((1, seqs), f32), (at, got))


def solution(mesh):
    split = Mesh(mesh.devices.reshape(2, mesh.shape["seq"] // 32, 4, 4, 2, 2), EVERY)
    placed = (
        P(SEQ, None, TP),
        P(SEQ, None, TP),
        P(None, TP),
        P(None, TP),
        P(None, TP),
        P(TP, None),
    )

    return jax.shard_map(
        on_device, mesh=split, in_specs=placed, out_specs=P(SEQ, None), check_vma=False
    )
```

```python
import jax
import jax.numpy as jnp
import numpy as np
from jax import lax
from jax.experimental import pallas as pl
from jax.experimental.pallas import tpu as pltpu
from jax.sharding import Mesh
from jax.sharding import PartitionSpec as P


HEADS = 32
KV_HEADS = 8
HEAD_DIM = 64
LANES = 128
SEQ = ("zb", "za", "x", "y")
NEAR = ("za", "x", "y")
TP = ("h", "c")
EVERY = SEQ + TP
SWAP = ((0, 1), (1, 0))

theta_base = 500000.0


def swapped(value, axis):
    return lax.ppermute(value, axis, SWAP)


def rope_tables(length, head_dim):
    half_dim = head_dim // 2
    steps = np.arange(half_dim, dtype=np.float32) * np.float32(2.0) / np.float32(head_dim)
    freqs_k = np.power(np.float32(theta_base), -steps)
    angles = np.arange(length, dtype=np.float32)[:, None] * freqs_k[None, :]
    sine = np.sin(angles)
    cos = np.tile(np.cos(angles), (1, LANES // half_dim))
    return cos, np.tile(np.concatenate([-sine, sine], axis=1), (1, LANES // head_dim))


def dot(left, right, dims=((1,), (0,))):
    return lax.dot_general(left, right, (dims, ((), ())), preferred_element_type=jnp.float32)


def kernel_call(body, outs, ins, scratch=(), vmem_mib=20, far=()):
    ins = [pltpu.with_memory_space_constraint(a, pltpu.HBM) if i in far else a for i, a in enumerate(ins)]
    hbm = pl.BlockSpec(memory_space=pltpu.HBM)
    smem = pl.BlockSpec(memory_space=pltpu.SMEM)
    vmem = pl.BlockSpec(memory_space=pltpu.VMEM)
    return pl.pallas_call(
        body,
        out_shape=outs,
        in_specs=[
            hbm if i in far else smem if a.dtype == jnp.int32 else vmem for i, a in enumerate(ins)
        ],
        out_specs=jax.tree.map(lambda _: vmem, outs),
        scratch_shapes=scratch,
        compiler_params=pltpu.CompilerParams(vmem_limit_bytes=vmem_mib * 2**20),
    )(*ins)


def lower_half(shape):
    return lax.broadcasted_iota(jnp.int32, shape, 1) % (2 * HEAD_DIM) < HEAD_DIM


def doubled(pair, low):
    turned = pltpu.roll(pair, HEAD_DIM, 1)
    return jnp.where(low, pair, turned), jnp.where(low, turned, pair)


def places_of(at):
    h, c = at[0], at[1]
    return [2 * h + c, 2 * h + 1 - c, 2 * (1 - h) + c, 2 * (1 - h) + 1 - c]


def rows_at(place, size):
    return pl.ds(pl.multiple_of(place * size, size), size)


def start_body(
    at, s0, s1, c0, c1, wq, wk, wv, wo, s_out, c_out, wq_out, wk_out, wv_out, wo_out, sums, grads, sems
):
    moves = [
        pltpu.make_async_copy(src, dst, sems.at[i])
        for i, (src, dst) in enumerate(
            ((wq, wq_out), (wk, wk_out), (wv, wv_out), (wo, wo_out), (s0, s_out), (c0, c_out))
        )
    ]
    for move in moves:
        move.start()
    for move in moves:
        move.wait()
    quarter = s_out.shape[1]
    near = places_of(at)[:2]
    begin = 0
    for w in (wq_out, wk_out, wv_out):
        end = begin + w.shape[1]
        sums[:, begin:end] = dot(s_out[...], w[rows_at(near[0], quarter), :]) + dot(
            s1[...], w[rows_at(near[1], quarter), :]
        )
        begin = end
    nt = ((1,), (1,))
    grads[...] = dot(c_out[...], wo_out[:, rows_at(near[0], quarter)], nt) + dot(
        c1[...], wo_out[:, rows_at(near[1], quarter)], nt
    )


def attention_body(at, s2, s3, wq, wk, wv, sums, cos_ref, sine_ref, attended, probs):
    quarter = s2.shape[1]
    far = places_of(at)[2:]

    def project(w, begin):
        total = sums[:, begin : begin + w.shape[1]]
        for part, place in zip((s2, s3), far):
            total = total + dot(part[...], w[rows_at(place, quarter), :])
        return total

    cos, sine = cos_ref[...], sine_ref[...]
    length = cos.shape[0]
    lane = lax.broadcasted_iota(jnp.int32, cos.shape, 1)
    first = lane % HEAD_DIM < HEAD_DIM // 2
    low = lower_half(cos.shape)

    def rotate(tile):
        ahead = pltpu.roll(tile, LANES - HEAD_DIM // 2, 1)
        behind = pltpu.roll(tile, HEAD_DIM // 2, 1)
        return tile * cos + jnp.where(first, ahead, behind) * sine

    width = wq.shape[1]
    keys = [k.astype(jnp.bfloat16) for k in doubled(rotate(project(wk, width)), low)]
    values = [v.astype(jnp.bfloat16) for v in doubled(project(wv, width + LANES), low)]
    queries = project(wq, 0)
    causal = lax.broadcasted_iota(jnp.int32, (length, length), 0) >= lax.broadcasted_iota(
        jnp.int32, (length, length), 1
    )
    for t in range(width // LANES):
        group = 2 * t // (HEADS // KV_HEADS)
        query = rotate(queries[:, t * LANES : (t + 1) * LANES])
        found = []
        for s in range(2):
            mine = low if s == 0 else jnp.logical_not(low)
            q = jnp.where(mine, query, 0.0).astype(jnp.bfloat16)
            scores = dot(q, keys[group], ((1,), (1,))) * HEAD_DIM ** (-0.5)
            scores = jnp.where(causal, scores, -jnp.inf)
            e = jnp.exp(scores - jnp.max(scores, axis=1, keepdims=True))
            p = (e / jnp.sum(e, axis=1, keepdims=True)).astype(jnp.bfloat16)
            probs[(2 * t + s) * length : (2 * t + s + 1) * length, :] = p
            found.append(dot(p, values[group]))
        tile = jnp.where(low, found[0], found[1])
        attended[:, t * LANES : (t + 1) * LANES] = tile.astype(jnp.bfloat16)


def put_blocks(blocks, turned, kind_rows, cols, col_at):
    tall = blocks.shape[1]
    begin, end = kind_rows
    wide = cols.shape[1] // LANES
    across = 8
    product = dot(turned, cols).astype(jnp.bfloat16)
    row = begin
    while row < end:
        block_row = row // tall
        stop = min(end, (block_row + 1) * tall)
        for j in range(wide):
            blocks[block_row * across + col_at + j, row - block_row * tall : stop - block_row * tall, :] = product[
                row - begin : stop - begin, j * LANES : (j + 1) * LANES
            ]
        row = stop


def grads_body(at, c2, c3, wo, partial, attended, probs, factors):
    length, quarter = c2.shape
    grads = partial[...]
    for part, place in zip((c2, c3), places_of(at)[2:]):
        grads = grads + dot(part[...], wo[:, rows_at(place, quarter)], ((1,), (1,)))
    low = lower_half((length, LANES))
    group_size = HEADS // KV_HEADS
    sums = []
    for g in range(2):
        stacked = []
        for t in range(g * group_size // 2, (g + 1) * group_size // 2):
            tile = grads[:, t * LANES : (t + 1) * LANES]
            stacked.append(jnp.where(low, tile, 0.0).astype(jnp.bfloat16))
            stacked.append(jnp.where(low, 0.0, tile).astype(jnp.bfloat16))
        rows = group_size * length
        found = dot(probs[g * rows : (g + 1) * rows, :], jnp.concatenate(stacked, 0), ((0,), (0,)))
        sums.append(found + pltpu.roll(found, HEAD_DIM, 1))
    width = attended.shape[1]
    factors[:, :width] = attended[...]
    factors[:, width:] = jnp.where(low, sums[0], sums[1]).astype(jnp.bfloat16)


def put_all(at, factors, cots, states, blocks):
    width = factors.shape[1] - LANES
    turned_a = factors[:, :width].T
    turned_v = factors[:, width:].T
    for k, (cot, state) in enumerate(zip(cots, states)):
        col_at = jnp.where(at[1] == 1, 1 - k, k) * (cot.shape[1] // LANES)
        put_blocks(blocks, turned_a, (0, width), cot, col_at)
        put_blocks(blocks, turned_v, (width, width + LANES), state, col_at)


def own_body(at, s0, s1, s2, s3, c0, c1, c2, c3, factors, blocks):
    here = at[0] == at[2]

    def half(*parts):
        return [jnp.where(here, parts[k][...], parts[k + 2][...]) for k in range(2)]

    put_all(at, factors, half(c0, c1, c2, c3), half(s0, s1, s2, s3), blocks)


def pick_body(at, own, far, piece):
    piece[...] = jnp.where(at[0] == at[2], far[...], own[...])


def other_body(at, s0, s1, c0, c1, factors, own_blocks, blocks):
    tall = own_blocks.shape[1]
    blocks[:, :tall, :] = own_blocks[...]
    put_all(at, factors, (c0[...], c1[...]), (s0[...], s1[...]), blocks.at[:, tall:, :])


def share_body(at, got, rows_out, wide):
    seqs, both, _ = got.shape
    tall = both // 2
    straight = at[2] == 0
    for s in range(seqs):
        wide[pl.ds(s * both, both), :] = got[s].astype(jnp.float32)

    def rows_of(r):
        found = [
            wide[pl.ds(r + k * tall, seqs, stride=both), :].astype(jnp.bfloat16) for k in range(2)
        ]
        return jnp.concatenate(
            [jnp.where(straight, found[0], found[1]), jnp.where(straight, found[1], found[0])], axis=0
        )

    total = jnp.zeros((2 * seqs, 2 * seqs), jnp.float32)
    for r in range(0, tall, 2):
        x = jnp.concatenate([rows_of(r), rows_of(r + 1)], axis=1)
        total = total + dot(x, x, ((1,), (1,)))
    eye = lax.broadcasted_iota(jnp.int32, total.shape, 0) == lax.broadcasted_iota(
        jnp.int32, total.shape, 1
    )
    diag = jnp.sum(jnp.where(eye, total, 0.0), axis=0, keepdims=True)
    rows = jnp.concatenate([total, jnp.broadcast_to(diag, total.shape)], axis=1)
    copies = rows_out.shape[0] // rows.shape[0]
    for k in range(copies):
        rows_out[pl.ds(k, rows.shape[0], stride=copies), :] = rows


def final_body(at, got, out):
    seqs = out.shape[1]
    total = jnp.sum(got[...], axis=0, keepdims=True)
    lane = lax.broadcasted_iota(jnp.int32, total.shape, 1)
    own_diag = jnp.sum(jnp.where(lane == at[3] + seqs, total, 0.0), axis=1, keepdims=True)
    diag = pltpu.roll(total, seqs, 1)
    out[...] = (total / jnp.sqrt(own_diag * diag))[:, :seqs]


def on_device(states, cotangent, wq, wk, wv, wo):
    bf16, f32 = jnp.bfloat16, jnp.float32
    shape = jax.ShapeDtypeStruct
    length, part = states.shape[1:]
    states, cotangent = states[0], cotangent[0]
    axes = (lax.axis_index("h"), lax.axis_index("c"), lax.axis_index("zb"), lax.axis_index(SEQ))
    at = jnp.stack(axes).astype(jnp.int32)
    blocks = lax.axis_size(NEAR)
    seqs = 2 * blocks
    tall = (part + LANES) * (2 * part) // (LANES * blocks)
    block_shape = shape((blocks, tall, LANES), bf16)

    def gathered(own):
        far = swapped(own, "h")
        near = swapped(own, "c")
        return near, far, swapped(far, "c")

    s1, s2, s3 = gathered(states)
    c1, c2, c3 = gathered(cotangent)
    cos, sine = rope_tables(length, HEAD_DIM)
    kv = wk.shape[1]
    s0, c0, wq, wk, wv, wo, sums, grads = kernel_call(
        start_body,
        (
            *(shape(a.shape, bf16) for a in (states, cotangent, wq, wk, wv, wo)),
            shape((length, part + 2 * kv), f32),
            shape((length, part), f32),
        ),
        (at, states, s1, cotangent, c1, wq, wk, wv, wo),
        (pltpu.SemaphoreType.DMA((6,)),),
        far=(1, 3, 5, 6, 7, 8),
    )

    def partner(own, far):
        piece = kernel_call(pick_body, shape(far.shape, bf16), (at, own, far))
        piece = swapped(piece, "zb")
        return piece, swapped(piece, "c")

    s_pieces = partner(s0, s2)
    c_pieces = partner(c0, c2)
    attended, probs = kernel_call(
        attention_body,
        (shape((length, part), bf16), shape((part // HEAD_DIM * length, length), bf16)),
        (at, s2, s3, wq, wk, wv, sums, cos, sine),
    )
    factors = kernel_call(
        grads_body, shape((length, part + LANES), bf16), (at, c2, c3, wo, grads, attended, probs)
    )
    other_factors = swapped(factors, "zb")
    own_blocks = kernel_call(own_body, block_shape, (at, s0, s1, s2, s3, c0, c1, c2, c3, factors))
    sent = kernel_call(
        other_body,
        shape((blocks, 2 * tall, LANES), bf16),
        (at, *s_pieces, *c_pieces, other_factors, own_blocks),
    )
    got = lax.all_to_all(sent, NEAR, 0, 0, tiled=True)
    copies = lax.axis_size(TP)
    rows = kernel_call(
        share_body,
        shape((seqs * copies, 2 * seqs), f32),
        (at, got),
        (pltpu.VMEM((seqs * tall, LANES), f32),),
    )
    rows = rows.reshape(seqs * copies, 1, 2 * seqs)
    got = lax.all_to_all(rows, EVERY, 0, 0, tiled=True).reshape(seqs * copies, 2 * seqs)
    return kernel_call(final_body, shape((1, seqs), f32), (at, got))


def solution(mesh):
    split = Mesh(mesh.devices.reshape(2, mesh.shape["seq"] // 32, 4, 4, 2, 2), EVERY)
    placed = (
        P(SEQ, None, TP),
        P(SEQ, None, TP),
        P(None, TP),
        P(None, TP),
        P(None, TP),
        P(TP, None),
    )

    return jax.shard_map(
        on_device, mesh=split, in_specs=placed, out_specs=P(SEQ, None), check_vma=False
    )
```

```python
import jax
import jax.numpy as jnp
import numpy as np
from jax import lax
from jax.experimental import pallas as pl
from jax.experimental.pallas import tpu as pltpu
from jax.sharding import Mesh
from jax.sharding import PartitionSpec as P


HEADS = 32
KV_HEADS = 8
HEAD_DIM = 64
LANES = 128
SEQ = ("zb", "za", "x", "y")
NEAR = ("za", "x", "y")
TP = ("h", "c")
EVERY = SEQ + TP
SWAP = ((0, 1), (1, 0))

theta_base = 500000.0


def swapped(value, axis):
    return lax.ppermute(value, axis, SWAP)


def rope_tables(length, head_dim):
    half_dim = head_dim // 2
    steps = np.arange(half_dim, dtype=np.float32) * np.float32(2.0) / np.float32(head_dim)
    freqs_k = np.power(np.float32(theta_base), -steps)
    angles = np.arange(length, dtype=np.float32)[:, None] * freqs_k[None, :]
    sine = np.sin(angles)
    cos = np.tile(np.cos(angles), (1, LANES // half_dim))
    return cos, np.tile(np.concatenate([-sine, sine], axis=1), (1, LANES // head_dim))


def dot(left, right, dims=((1,), (0,))):
    return lax.dot_general(left, right, (dims, ((), ())), preferred_element_type=jnp.float32)


def kernel_call(body, outs, ins, scratch=(), vmem_mib=16, far=()):
    ins = [pltpu.with_memory_space_constraint(a, pltpu.HBM) if i in far else a for i, a in enumerate(ins)]
    hbm = pl.BlockSpec(memory_space=pltpu.HBM)
    smem = pl.BlockSpec(memory_space=pltpu.SMEM)
    vmem = pl.BlockSpec(memory_space=pltpu.VMEM)
    return pl.pallas_call(
        body,
        out_shape=outs,
        in_specs=[
            hbm if i in far else smem if a.dtype == jnp.int32 else vmem for i, a in enumerate(ins)
        ],
        out_specs=jax.tree.map(lambda _: vmem, outs),
        scratch_shapes=scratch,
        compiler_params=pltpu.CompilerParams(vmem_limit_bytes=vmem_mib * 2**20),
    )(*ins)


def lower_half(shape):
    return lax.broadcasted_iota(jnp.int32, shape, 1) % (2 * HEAD_DIM) < HEAD_DIM


def doubled(pair, low):
    turned = pltpu.roll(pair, HEAD_DIM, 1)
    return jnp.where(low, pair, turned), jnp.where(low, turned, pair)


def places_of(at):
    h, c = at[0], at[1]
    return [2 * h + c, 2 * h + 1 - c, 2 * (1 - h) + c, 2 * (1 - h) + 1 - c]


def rows_at(place, size):
    return pl.ds(pl.multiple_of(place * size, size), size)


def start_body(
    at, s0, s1, c0, c1, wq, wk, wv, wo, s_out, c_out, wq_out, wk_out, wv_out, wo_out, sums, grads, sems
):
    moves = [
        pltpu.make_async_copy(src, dst, sems.at[i])
        for i, (src, dst) in enumerate(
            ((wq, wq_out), (wk, wk_out), (wv, wv_out), (wo, wo_out), (s0, s_out), (c0, c_out))
        )
    ]
    for move in moves:
        move.start()
    for move in moves:
        move.wait()
    quarter = s_out.shape[1]
    near = places_of(at)[:2]
    begin = 0
    for w in (wq_out, wk_out, wv_out):
        end = begin + w.shape[1]
        sums[:, begin:end] = dot(s_out[...], w[rows_at(near[0], quarter), :]) + dot(
            s1[...], w[rows_at(near[1], quarter), :]
        )
        begin = end
    nt = ((1,), (1,))
    grads[...] = dot(c_out[...], wo_out[:, rows_at(near[0], quarter)], nt) + dot(
        c1[...], wo_out[:, rows_at(near[1], quarter)], nt
    )


def attention_body(
    at, s0, s2, s3, wq, wk, wv, sums, cos_ref, sine_ref, attended, probs, piece
):
    piece[...] = jnp.where(at[0] == at[2], s2[...], s0[...])
    quarter = s2.shape[1]
    far = places_of(at)[2:]

    def project(w, begin):
        total = sums[:, begin : begin + w.shape[1]]
        for part, place in zip((s2, s3), far):
            total = total + dot(part[...], w[rows_at(place, quarter), :])
        return total

    cos, sine = cos_ref[...], sine_ref[...]
    length = cos.shape[0]
    lane = lax.broadcasted_iota(jnp.int32, cos.shape, 1)
    first = lane % HEAD_DIM < HEAD_DIM // 2
    low = lower_half(cos.shape)

    def rotate(tile):
        ahead = pltpu.roll(tile, LANES - HEAD_DIM // 2, 1)
        behind = pltpu.roll(tile, HEAD_DIM // 2, 1)
        return tile * cos + jnp.where(first, ahead, behind) * sine

    width = wq.shape[1]
    keys = [k.astype(jnp.bfloat16) for k in doubled(rotate(project(wk, width)), low)]
    values = [v.astype(jnp.bfloat16) for v in doubled(project(wv, width + LANES), low)]
    queries = project(wq, 0)
    causal = lax.broadcasted_iota(jnp.int32, (length, length), 0) >= lax.broadcasted_iota(
        jnp.int32, (length, length), 1
    )
    for t in range(width // LANES):
        group = 2 * t // (HEADS // KV_HEADS)
        query = rotate(queries[:, t * LANES : (t + 1) * LANES])
        found = []
        for s in range(2):
            mine = low if s == 0 else jnp.logical_not(low)
            q = jnp.where(mine, query, 0.0).astype(jnp.bfloat16)
            scores = dot(q, keys[group], ((1,), (1,))) * HEAD_DIM ** (-0.5)
            scores = jnp.where(causal, scores, -jnp.inf)
            e = jnp.exp(scores - jnp.max(scores, axis=1, keepdims=True))
            p = (e / jnp.sum(e, axis=1, keepdims=True)).astype(jnp.bfloat16)
            probs[(2 * t + s) * length : (2 * t + s + 1) * length, :] = p
            found.append(dot(p, values[group]))
        tile = jnp.where(low, found[0], found[1])
        attended[:, t * LANES : (t + 1) * LANES] = tile.astype(jnp.bfloat16)


def put_blocks(blocks, turned, kind_rows, cols, col_at):
    tall = blocks.shape[1]
    begin, end = kind_rows
    wide = cols.shape[1] // LANES
    across = 8
    product = dot(turned, cols).astype(jnp.bfloat16)
    row = begin
    while row < end:
        block_row = row // tall
        stop = min(end, (block_row + 1) * tall)
        for j in range(wide):
            blocks[block_row * across + col_at + j, row - block_row * tall : stop - block_row * tall, :] = product[
                row - begin : stop - begin, j * LANES : (j + 1) * LANES
            ]
        row = stop


def grads_body(at, c0, c2, c3, wo, partial, attended, probs, packed):
    length, quarter = c2.shape
    grads = partial[...]
    for part, place in zip((c2, c3), places_of(at)[2:]):
        grads = grads + dot(part[...], wo[:, rows_at(place, quarter)], ((1,), (1,)))
    low = lower_half((length, LANES))
    group_size = HEADS // KV_HEADS
    sums = []
    for g in range(2):
        stacked = []
        for t in range(g * group_size // 2, (g + 1) * group_size // 2):
            tile = grads[:, t * LANES : (t + 1) * LANES]
            stacked.append(jnp.where(low, tile, 0.0).astype(jnp.bfloat16))
            stacked.append(jnp.where(low, 0.0, tile).astype(jnp.bfloat16))
        rows = group_size * length
        found = dot(probs[g * rows : (g + 1) * rows, :], jnp.concatenate(stacked, 0), ((0,), (0,)))
        sums.append(found + pltpu.roll(found, HEAD_DIM, 1))
    width = attended.shape[1]
    packed[:, :width] = attended[...]
    packed[:, width : width + LANES] = jnp.where(low, sums[0], sums[1]).astype(jnp.bfloat16)
    packed[:, width + LANES :] = jnp.where(at[0] == at[2], c2[...], c0[...])


def put_all(at, packed, cots, states, blocks):
    width = states[0].shape[1]
    turned_a = packed[:, :width].T
    turned_v = packed[:, width : width + LANES].T
    for k, (cot, state) in enumerate(zip(cots, states)):
        col_at = jnp.where(at[1] == 1, 1 - k, k) * (width // LANES)
        put_blocks(blocks, turned_a, (0, width), cot, col_at)
        put_blocks(blocks, turned_v, (width, width + LANES), state, col_at)


def own_body(at, s0, s1, s2, s3, c0, c1, c2, c3, packed, blocks):
    here = at[0] == at[2]

    def half(*parts):
        return [jnp.where(here, parts[k][...], parts[k + 2][...]) for k in range(2)]

    put_all(at, packed, half(c0, c1, c2, c3), half(s0, s1, s2, s3), blocks)


def other_body(at, s0, s1, packed, packed_near, blocks):
    begin = s0.shape[1] + LANES
    cots = (packed[:, begin:], packed_near[:, begin:])
    put_all(at, packed, cots, (s0[...], s1[...]), blocks)


def turn_blocks(got, wide, keep, ready=lambda: None):
    seqs, tall, _ = got.shape
    for s in range(seqs):
        wide[pl.ds(s * tall, tall), :] = got[s].astype(jnp.float32)
    ready()
    for r in range(tall):
        keep(r, wide[pl.ds(r, seqs, stride=tall), :].astype(jnp.bfloat16))


def turn_body(got, turned, wide):
    def keep(r, rows):
        turned[r] = rows

    turn_blocks(got, wide, keep)


def share_body(at, own_far, other, rows_out, wide, own, sem):
    _, seqs, _ = own.shape
    fetch = pltpu.make_async_copy(own_far, own, sem)
    fetch.start()
    straight = at[2] == 0
    total = jnp.zeros((2 * seqs, 2 * seqs), jnp.float32)
    waiting = []

    def keep(r, rows):
        nonlocal total
        mine = own[r]
        waiting.append(
            jnp.concatenate([jnp.where(straight, mine, rows), jnp.where(straight, rows, mine)], axis=0)
        )
        if len(waiting) == 2:
            x = jnp.concatenate(waiting, axis=1)
            total = total + dot(x, x, ((1,), (1,)))
            waiting.clear()

    turn_blocks(other, wide, keep, fetch.wait)
    eye = lax.broadcasted_iota(jnp.int32, total.shape, 0) == lax.broadcasted_iota(
        jnp.int32, total.shape, 1
    )
    diag = jnp.sum(jnp.where(eye, total, 0.0), axis=0, keepdims=True)
    rows = jnp.concatenate([total, jnp.broadcast_to(diag, total.shape)], axis=1)
    copies = rows_out.shape[0] // rows.shape[0]
    for k in range(copies):
        rows_out[pl.ds(k, rows.shape[0], stride=copies), :] = rows


def final_body(at, got, out):
    seqs = out.shape[1]
    total = jnp.sum(got[...], axis=0, keepdims=True)
    lane = lax.broadcasted_iota(jnp.int32, total.shape, 1)
    own_diag = jnp.sum(jnp.where(lane == at[3] + seqs, total, 0.0), axis=1, keepdims=True)
    diag = pltpu.roll(total, seqs, 1)
    out[...] = (total / jnp.sqrt(own_diag * diag))[:, :seqs]


def on_device(states, cotangent, wq, wk, wv, wo):
    bf16, f32 = jnp.bfloat16, jnp.float32
    shape = jax.ShapeDtypeStruct
    length, part = states.shape[1:]
    states, cotangent = states[0], cotangent[0]
    axes = (lax.axis_index("h"), lax.axis_index("c"), lax.axis_index("zb"), lax.axis_index(SEQ))
    at = jnp.stack(axes).astype(jnp.int32)
    blocks = lax.axis_size(NEAR)
    seqs = 2 * blocks
    tall = (part + LANES) * (2 * part) // (LANES * blocks)
    block_shape = shape((blocks, tall, LANES), bf16)
    wide = pltpu.VMEM((blocks * tall, LANES), f32)

    def gathered(own):
        far = swapped(own, "h")
        near = swapped(own, "c")
        return near, far, swapped(far, "c")

    s1, s2, s3 = gathered(states)
    c1, c2, c3 = gathered(cotangent)
    cos, sine = rope_tables(length, HEAD_DIM)
    kv = wk.shape[1]
    s0, c0, wq, wk, wv, wo, sums, grads = kernel_call(
        start_body,
        (
            *(shape(a.shape, bf16) for a in (states, cotangent, wq, wk, wv, wo)),
            shape((length, part + 2 * kv), f32),
            shape((length, part), f32),
        ),
        (at, states, s1, cotangent, c1, wq, wk, wv, wo),
        (pltpu.SemaphoreType.DMA((6,)),),
        far=(1, 3, 5, 6, 7, 8),
    )
    attended, probs, s_piece = kernel_call(
        attention_body,
        (
            shape((length, part), bf16),
            shape((part // HEAD_DIM * length, length), bf16),
            shape((length, part), bf16),
        ),
        (at, s0, s2, s3, wq, wk, wv, sums, cos, sine),
    )
    s_piece = swapped(s_piece, "zb")
    packed = kernel_call(
        grads_body,
        shape((length, 2 * part + LANES), bf16),
        (at, c0, c2, c3, wo, grads, attended, probs),
    )
    other_packed = swapped(packed, "zb")
    own_blocks = kernel_call(own_body, block_shape, (at, s0, s1, s2, s3, c0, c1, c2, c3, packed))
    got_own = lax.all_to_all(own_blocks, NEAR, 0, 0, tiled=True)
    s_near = swapped(s_piece, "c")
    packed_near = swapped(other_packed, "c")
    other_blocks = kernel_call(
        other_body, block_shape, (at, s_piece, s_near, other_packed, packed_near)
    )
    got_other = lax.all_to_all(other_blocks, NEAR, 0, 0, tiled=True)
    own_turned = kernel_call(turn_body, shape((tall, blocks, LANES), bf16), (got_own,), (wide,))
    copies = lax.axis_size(TP)
    rows = kernel_call(
        share_body,
        shape((seqs * copies, 2 * seqs), f32),
        (at, own_turned, got_other),
        (wide, pltpu.VMEM(own_turned.shape, bf16), pltpu.SemaphoreType.DMA),
        far=(1,),
    )
    rows = rows.reshape(seqs * copies, 1, 2 * seqs)
    got = lax.all_to_all(rows, EVERY, 0, 0, tiled=True).reshape(seqs * copies, 2 * seqs)
    return kernel_call(final_body, shape((1, seqs), f32), (at, got))


def solution(mesh):
    split = Mesh(mesh.devices.reshape(2, mesh.shape["seq"] // 32, 4, 4, 2, 2), EVERY)
    placed = (
        P(SEQ, None, TP),
        P(SEQ, None, TP),
        P(None, TP),
        P(None, TP),
        P(None, TP),
        P(TP, None),
    )

    return jax.shard_map(
        on_device, mesh=split, in_specs=placed, out_specs=P(SEQ, None), check_vma=False
    )
```

```python
import functools

import functools

import jax
import jax.numpy as jnp
import numpy as np
from jax import lax
from jax.experimental import pallas as pl
from jax.experimental.pallas import tpu as pltpu
from jax.sharding import Mesh
from jax.sharding import PartitionSpec as P


HEAD_DIM = 64
LANES = 128
SEQ = ("zb", "za", "x", "y")
NEAR = ("za", "x", "y")
TP = ("h", "c")
EVERY = SEQ + TP
SWAP = ((0, 1), (1, 0))


theta_base = 500000.0


def swapped(value, axis):
    return lax.ppermute(value, axis, SWAP)


def rope_tables(length, head_dim):
    half_dim = head_dim // 2
    steps = np.arange(half_dim, dtype=np.float32) * np.float32(2.0) / np.float32(head_dim)
    freqs_k = np.power(np.float32(theta_base), -steps)
    angles = np.arange(length, dtype=np.float32)[:, None] * freqs_k[None, :]
    sine = np.sin(angles)
    cos = np.tile(np.cos(angles), (1, LANES // half_dim))
    return cos, np.tile(np.concatenate([-sine, sine], axis=1), (1, LANES // head_dim))


def dot(left, right, dims=((1,), (0,))):
    return lax.dot_general(left, right, (dims, ((), ())), preferred_element_type=jnp.float32)


def kernel_call(body, outs, ins, scratch=(), vmem_mib=20, far=()):
    ins = [pltpu.with_memory_space_constraint(a, pltpu.HBM) if i in far else a for i, a in enumerate(ins)]
    hbm = pl.BlockSpec(memory_space=pltpu.HBM)
    smem = pl.BlockSpec(memory_space=pltpu.SMEM)
    vmem = pl.BlockSpec(memory_space=pltpu.VMEM)
    return pl.pallas_call(
        body,
        out_shape=outs,
        in_specs=[
            hbm if i in far else smem if a.dtype == jnp.int32 else vmem for i, a in enumerate(ins)
        ],
        out_specs=jax.tree.map(lambda _: vmem, outs),
        scratch_shapes=scratch,
        compiler_params=pltpu.CompilerParams(vmem_limit_bytes=vmem_mib * 2**20),
    )(*ins)


def lower_half(shape):
    return lax.broadcasted_iota(jnp.int32, shape, 1) % (2 * HEAD_DIM) < HEAD_DIM


def doubled(pair, low):
    turned = pltpu.roll(pair, HEAD_DIM, 1)
    return jnp.where(low, pair, turned), jnp.where(low, turned, pair)


def rows_at(place, size):
    return pl.ds(pl.multiple_of(place * size, size), size)


def places_of(at):
    h, c = at[0], at[1]
    return [2 * h + c, 2 * h + 1 - c, 2 * (1 - h) + c, 2 * (1 - h) + 1 - c]


def own_quarters(parts):
    values = [part[...] for part in parts]
    far = [jnp.concatenate([values[2 + k], values[4 + k]], axis=0) for k in range(2)]
    return values[:2] + far


def partner_quarters(at, parts):
    straight = at[2] == 0
    values = [part[...] for part in parts]
    up, down = values[:2], values[2:]
    here = [jnp.where(straight, d, u) for u, d in zip(up, down)]
    return here + [jnp.where(straight, u, d) for u, d in zip(up, down)]


def fetch_body(at, wq, wk, wv, wo, wq_out, wk_out, wv_out, wo_out, sems):
    part = wq_out.shape[1]
    half = rows_at(at[2], part)
    moves = [
        pltpu.make_async_copy(src, dst, sems.at[i])
        for i, (src, dst) in enumerate(
            ((wq.at[:, half], wq_out), (wk, wk_out), (wv, wv_out), (wo.at[half, :], wo_out))
        )
    ]
    for move in moves:
        move.start()
    for move in moves:
        move.wait()


def attention_body(partner, at, *refs):
    *found, wq, wk, wv, cos_ref, sine_ref, attended, probs = refs
    parts = partner_quarters(at, found) if partner else own_quarters(found)
    quarter = parts[0].shape[1]

    def project(w):
        total = None
        for part, place in zip(parts, places_of(at)):
            term = dot(part, w[rows_at(place, quarter), :])
            total = term if total is None else total + term
        return total

    cos, sine = cos_ref[...], sine_ref[...]
    length = cos.shape[0]
    lane = lax.broadcasted_iota(jnp.int32, cos.shape, 1)
    first = lane % HEAD_DIM < HEAD_DIM // 2
    low = lower_half(cos.shape)
    straight = at[2] == 0

    def rotate(tile):
        ahead = pltpu.roll(tile, LANES - HEAD_DIM // 2, 1)
        behind = pltpu.roll(tile, HEAD_DIM // 2, 1)
        return tile * cos + jnp.where(first, ahead, behind) * sine

    def own_head(tile):
        even, odd = doubled(tile, low)
        return jnp.where(straight, even, odd).astype(jnp.bfloat16)

    keys, values, queries = own_head(rotate(project(wk))), own_head(project(wv)), project(wq)
    causal = lax.broadcasted_iota(jnp.int32, (length, length), 0) >= lax.broadcasted_iota(
        jnp.int32, (length, length), 1
    )
    for t in range(queries.shape[1] // LANES):
        query = rotate(queries[:, t * LANES : (t + 1) * LANES])
        found = []
        for s in range(2):
            mine = low if s == 0 else jnp.logical_not(low)
            q = jnp.where(mine, query, 0.0).astype(jnp.bfloat16)
            scores = dot(q, keys, ((1,), (1,))) * HEAD_DIM ** (-0.5)
            scores = jnp.where(causal, scores, -jnp.inf)
            e = jnp.exp(scores - jnp.max(scores, axis=1, keepdims=True))
            p = (e / jnp.sum(e, axis=1, keepdims=True)).astype(jnp.bfloat16)
            probs[(2 * t + s) * length : (2 * t + s + 1) * length, :] = p
            found.append(dot(p, values))
        tile = jnp.where(low, found[0], found[1])
        attended[:, t * LANES : (t + 1) * LANES] = tile.astype(jnp.bfloat16)


def blocks_body(at, *refs):
    s_refs, c_refs = refs[:10], refs[10:20]
    wo, attended_own, probs_own, attended_partner, probs_partner, blocks = refs[20:]
    attended, probs = (attended_own, attended_partner), (probs_own, probs_partner)
    states = list(zip(own_quarters(s_refs[:6]), partner_quarters(at, s_refs[6:])))
    cots = list(zip(own_quarters(c_refs[:6]), partner_quarters(at, c_refs[6:])))
    places = places_of(at)
    length, quarter = states[0][0].shape
    grads = None
    for pair, place in zip(cots, places):
        term = dot(jnp.concatenate(pair, axis=0), wo[:, rows_at(place, quarter)], ((1,), (1,)))
        grads = term if grads is None else grads + term
    low = lower_half((length, LANES))
    width = attended_own.shape[1]
    tiles = width // LANES
    tall = blocks.shape[1] // 2
    across = 4 * quarter // LANES
    for n in range(2):
        rows = slice(n * length, (n + 1) * length)
        stacked = []
        for t in range(tiles):
            tile = grads[rows, t * LANES : (t + 1) * LANES]
            stacked.append(jnp.where(low, tile, 0.0).astype(jnp.bfloat16))
            stacked.append(jnp.where(low, 0.0, tile).astype(jnp.bfloat16))
        found = dot(probs[n][...], jnp.concatenate(stacked, 0), ((0,), (0,)))
        value_gradient = (found + pltpu.roll(found, HEAD_DIM, 1)).astype(jnp.bfloat16)
        turned_a = attended[n][...].T
        turned_v = value_gradient.T[:HEAD_DIM, :]
        for k, place in enumerate(places):
            upper = dot(turned_a, cots[k][n]).astype(jnp.bfloat16)
            lower = dot(turned_v, states[k][n]).astype(jnp.bfloat16)
            for j in range(quarter // LANES):
                cols = slice(j * LANES, (j + 1) * LANES)
                at_col = place * (quarter // LANES) + j
                begin = n * tall
                blocks[at_col, begin : begin + tall, :] = upper[:tall, cols]
                rest = width - tall
                blocks[across + at_col, begin : begin + rest, :] = upper[tall:, cols]
                blocks[across + at_col, begin + rest : begin + tall, :] = lower[:, cols]


def share_body(at, got, rows_out, wide):
    seqs, both, _ = got.shape
    tall = both // 2
    straight = at[2] == 0
    for s in range(seqs):
        wide[pl.ds(s * both, both), :] = got[s].astype(jnp.float32)

    def rows_of(r):
        found = [
            wide[pl.ds(r + k * tall, seqs, stride=both), :].astype(jnp.bfloat16) for k in range(2)
        ]
        return jnp.concatenate(
            [jnp.where(straight, found[0], found[1]), jnp.where(straight, found[1], found[0])], axis=0
        )

    total = jnp.zeros((2 * seqs, 2 * seqs), jnp.float32)
    for r in range(0, tall, 2):
        x = jnp.concatenate([rows_of(r), rows_of(r + 1)], axis=1)
        total = total + dot(x, x, ((1,), (1,)))
    eye = lax.broadcasted_iota(jnp.int32, total.shape, 0) == lax.broadcasted_iota(
        jnp.int32, total.shape, 1
    )
    diag = jnp.sum(jnp.where(eye, total, 0.0), axis=0, keepdims=True)
    rows = jnp.concatenate([total, jnp.broadcast_to(diag, total.shape)], axis=1)
    copies = rows_out.shape[0] // rows.shape[0]
    for k in range(copies):
        rows_out[pl.ds(k, rows.shape[0], stride=copies), :] = rows


def final_body(at, got, out):
    seqs = out.shape[1]
    total = jnp.sum(got[...], axis=0, keepdims=True)
    lane = lax.broadcasted_iota(jnp.int32, total.shape, 1)
    own_diag = jnp.sum(jnp.where(lane == at[3] + seqs, total, 0.0), axis=1, keepdims=True)
    diag = pltpu.roll(total, seqs, 1)
    out[...] = (total / jnp.sqrt(own_diag * diag))[:, :seqs]


def on_device(states, cotangent, wq, wk, wv, wo):
    bf16, f32 = jnp.bfloat16, jnp.float32
    shape = jax.ShapeDtypeStruct
    length, part = states.shape[1:]
    states, cotangent = states[0], cotangent[0]
    axes = (lax.axis_index("h"), lax.axis_index("c"), lax.axis_index("zb"), lax.axis_index(SEQ))
    at = jnp.stack(axes).astype(jnp.int32)
    blocks = lax.axis_size(NEAR)
    seqs = 2 * blocks
    tall = (part + LANES) * (2 * part) // (LANES * blocks)

    def around(step):
        ring = (0, 2, 1, 3)
        return [(ring[q], ring[(q + step) % 4]) for q in range(4)]

    def moved(piece, step):
        return lax.ppermute(piece, ("zb", "h"), around(step))

    def near(piece):
        return piece, swapped(piece, "c")

    def gathered(own):
        up, down = moved(own, 1), moved(own, -1)
        half = length // 2
        low, high = moved(up[:half], 1), moved(down[half:], -1)
        kinds = (own, low, high, up, down)
        return [part for piece in kinds for part in near(piece)]

    s_parts, c_parts = gathered(states), gathered(cotangent)
    cos, sine = rope_tables(length, HEAD_DIM)
    width = part // 2
    wq, wk, wv, wo = kernel_call(
        fetch_body,
        tuple(
            shape(dims, bf16)
            for dims in ((wq.shape[0], width), wk.shape, wv.shape, (width, wo.shape[1]))
        ),
        (at, wq, wk, wv, wo),
        (pltpu.SemaphoreType.DMA((4,)),),
        far=(1, 2, 3, 4),
    )

    def attention(partner, parts):
        return kernel_call(
            functools.partial(attention_body, partner),
            (
                shape((length, width), bf16),
                shape((width // HEAD_DIM * length, length), bf16),
            ),
            (at, *parts, wq, wk, wv, cos, sine),
        )

    partner_found = attention(True, s_parts[6:])
    own_found = attention(False, s_parts[:6])
    sent = kernel_call(
        blocks_body,
        shape((blocks, 2 * tall, LANES), bf16),
        (at, *s_parts, *c_parts, wo, *own_found, *partner_found),
    )
    got = lax.all_to_all(sent, NEAR, 0, 0, tiled=True)
    copies = lax.axis_size(TP)
    rows = kernel_call(
        share_body,
        shape((seqs * copies, 2 * seqs), f32),
        (at, got),
        (pltpu.VMEM((seqs * tall, LANES), f32),),
    )
    rows = rows.reshape(seqs * copies, 1, 2 * seqs)
    got = lax.all_to_all(rows, EVERY, 0, 0, tiled=True).reshape(seqs * copies, 2 * seqs)
    return kernel_call(final_body, shape((1, seqs), f32), (at, got))


def solution(mesh):
    split = Mesh(mesh.devices.reshape(2, mesh.shape["seq"] // 32, 4, 4, 2, 2), EVERY)
    placed = (
        P(SEQ, None, TP),
        P(SEQ, None, TP),
        P(None, TP),
        P(None, TP),
        P(None, TP),
        P(TP, None),
    )

    return jax.shard_map(
        on_device, mesh=split, in_specs=placed, out_specs=P(SEQ, None), check_vma=False
    )
```

```python
import functools

import functools

import jax
import jax.numpy as jnp
import numpy as np
from jax import lax
from jax.experimental import pallas as pl
from jax.experimental.pallas import tpu as pltpu
from jax.sharding import Mesh
from jax.sharding import PartitionSpec as P


HEAD_DIM = 64
LANES = 128
SEQ = ("zb", "za", "x", "y")
NEAR = ("za", "x", "y")
TP = ("h", "c")
EVERY = SEQ + TP
SWAP = ((0, 1), (1, 0))


theta_base = 500000.0


def swapped(value, axis):
    return lax.ppermute(value, axis, SWAP)


def rope_tables(length, head_dim):
    half_dim = head_dim // 2
    steps = np.arange(half_dim, dtype=np.float32) * np.float32(2.0) / np.float32(head_dim)
    freqs_k = np.power(np.float32(theta_base), -steps)
    angles = np.arange(length, dtype=np.float32)[:, None] * freqs_k[None, :]
    sine = np.sin(angles)
    cos = np.tile(np.cos(angles), (1, LANES // half_dim))
    return cos, np.tile(np.concatenate([-sine, sine], axis=1), (1, LANES // head_dim))


def dot(left, right, dims=((1,), (0,))):
    return lax.dot_general(left, right, (dims, ((), ())), preferred_element_type=jnp.float32)


def kernel_call(body, outs, ins, scratch=(), vmem_mib=20, far=()):
    ins = [pltpu.with_memory_space_constraint(a, pltpu.HBM) if i in far else a for i, a in enumerate(ins)]
    hbm = pl.BlockSpec(memory_space=pltpu.HBM)
    smem = pl.BlockSpec(memory_space=pltpu.SMEM)
    vmem = pl.BlockSpec(memory_space=pltpu.VMEM)
    return pl.pallas_call(
        body,
        out_shape=outs,
        in_specs=[
            hbm if i in far else smem if a.dtype == jnp.int32 else vmem for i, a in enumerate(ins)
        ],
        out_specs=jax.tree.map(lambda _: vmem, outs),
        scratch_shapes=scratch,
        compiler_params=pltpu.CompilerParams(vmem_limit_bytes=vmem_mib * 2**20),
    )(*ins)


def lower_half(shape):
    return lax.broadcasted_iota(jnp.int32, shape, 1) % (2 * HEAD_DIM) < HEAD_DIM


def doubled(pair, low):
    turned = pltpu.roll(pair, HEAD_DIM, 1)
    return jnp.where(low, pair, turned), jnp.where(low, turned, pair)


def rows_at(place, size):
    return pl.ds(pl.multiple_of(place * size, size), size)


def places_of(at):
    h, c = at[0], at[1]
    return [2 * h + c, 2 * h + 1 - c, 2 * (1 - h) + c, 2 * (1 - h) + 1 - c]


def own_quarters(parts):
    return [part[...] for part in parts]


def partner_quarters(at, parts):
    straight = at[2] == 0
    values = [part[...] for part in parts]
    up, down = values[:2], values[2:]
    here = [jnp.where(straight, d, u) for u, d in zip(up, down)]
    return here + [jnp.where(straight, u, d) for u, d in zip(up, down)]


def fetch_body(at, wq, wk, wv, wo, wq_out, wk_out, wv_out, wo_out, sems):
    part = wq_out.shape[1]
    half = rows_at(at[2], part)
    moves = [
        pltpu.make_async_copy(src, dst, sems.at[i])
        for i, (src, dst) in enumerate(
            ((wq.at[:, half], wq_out), (wk, wk_out), (wv, wv_out), (wo.at[half, :], wo_out))
        )
    ]
    for move in moves:
        move.start()
    for move in moves:
        move.wait()


def attention_body(partner, at, *refs):
    *found, wq, wk, wv, cos_ref, sine_ref, attended, probs = refs
    parts = partner_quarters(at, found) if partner else own_quarters(found)
    quarter = parts[0].shape[1]

    def project(w):
        total = None
        for part, place in zip(parts, places_of(at)):
            term = dot(part, w[rows_at(place, quarter), :])
            total = term if total is None else total + term
        return total

    cos, sine = cos_ref[...], sine_ref[...]
    length = cos.shape[0]
    lane = lax.broadcasted_iota(jnp.int32, cos.shape, 1)
    first = lane % HEAD_DIM < HEAD_DIM // 2
    low = lower_half(cos.shape)
    straight = at[2] == 0

    def rotate(tile):
        ahead = pltpu.roll(tile, LANES - HEAD_DIM // 2, 1)
        behind = pltpu.roll(tile, HEAD_DIM // 2, 1)
        return tile * cos + jnp.where(first, ahead, behind) * sine

    def own_head(tile):
        even, odd = doubled(tile, low)
        return jnp.where(straight, even, odd).astype(jnp.bfloat16)

    keys, values, queries = own_head(rotate(project(wk))), own_head(project(wv)), project(wq)
    causal = lax.broadcasted_iota(jnp.int32, (length, length), 0) >= lax.broadcasted_iota(
        jnp.int32, (length, length), 1
    )
    for t in range(queries.shape[1] // LANES):
        query = rotate(queries[:, t * LANES : (t + 1) * LANES])
        found = []
        for s in range(2):
            mine = low if s == 0 else jnp.logical_not(low)
            q = jnp.where(mine, query, 0.0).astype(jnp.bfloat16)
            scores = dot(q, keys, ((1,), (1,))) * HEAD_DIM ** (-0.5)
            scores = jnp.where(causal, scores, -jnp.inf)
            e = jnp.exp(scores - jnp.max(scores, axis=1, keepdims=True))
            p = (e / jnp.sum(e, axis=1, keepdims=True)).astype(jnp.bfloat16)
            probs[(2 * t + s) * length : (2 * t + s + 1) * length, :] = p
            found.append(dot(p, values))
        tile = jnp.where(low, found[0], found[1])
        attended[:, t * LANES : (t + 1) * LANES] = tile.astype(jnp.bfloat16)


def blocks_body(at, *refs):
    s_refs, c_refs = refs[:8], refs[8:16]
    wo, attended_own, probs_own, attended_partner, probs_partner, blocks = refs[16:]
    attended, probs = (attended_own, attended_partner), (probs_own, probs_partner)
    states = list(zip(own_quarters(s_refs[:4]), partner_quarters(at, s_refs[4:])))
    cots = list(zip(own_quarters(c_refs[:4]), partner_quarters(at, c_refs[4:])))
    places = places_of(at)
    length, quarter = states[0][0].shape
    grads = None
    for pair, place in zip(cots, places):
        term = dot(jnp.concatenate(pair, axis=0), wo[:, rows_at(place, quarter)], ((1,), (1,)))
        grads = term if grads is None else grads + term
    low = lower_half((length, LANES))
    width = attended_own.shape[1]
    tiles = width // LANES
    tall = blocks.shape[1] // 2
    across = 4 * quarter // LANES
    for n in range(2):
        rows = slice(n * length, (n + 1) * length)
        stacked = []
        for t in range(tiles):
            tile = grads[rows, t * LANES : (t + 1) * LANES]
            stacked.append(jnp.where(low, tile, 0.0).astype(jnp.bfloat16))
            stacked.append(jnp.where(low, 0.0, tile).astype(jnp.bfloat16))
        found = dot(probs[n][...], jnp.concatenate(stacked, 0), ((0,), (0,)))
        value_gradient = (found + pltpu.roll(found, HEAD_DIM, 1)).astype(jnp.bfloat16)
        turned_a = attended[n][...].T
        turned_v = value_gradient.T[:HEAD_DIM, :]
        for k, place in enumerate(places):
            upper = dot(turned_a, cots[k][n]).astype(jnp.bfloat16)
            lower = dot(turned_v, states[k][n]).astype(jnp.bfloat16)
            for j in range(quarter // LANES):
                cols = slice(j * LANES, (j + 1) * LANES)
                at_col = place * (quarter // LANES) + j
                begin = n * tall
                blocks[at_col, begin : begin + tall, :] = upper[:tall, cols]
                rest = width - tall
                blocks[across + at_col, begin : begin + rest, :] = upper[tall:, cols]
                blocks[across + at_col, begin + rest : begin + tall, :] = lower[:, cols]


def share_body(at, got, rows_out, wide):
    seqs, both, _ = got.shape
    tall = both // 2
    straight = at[2] == 0
    for s in range(seqs):
        wide[pl.ds(s * both, both), :] = got[s].astype(jnp.float32)

    def rows_of(r):
        found = [
            wide[pl.ds(r + k * tall, seqs, stride=both), :].astype(jnp.bfloat16) for k in range(2)
        ]
        return jnp.concatenate(
            [jnp.where(straight, found[0], found[1]), jnp.where(straight, found[1], found[0])], axis=0
        )

    total = jnp.zeros((2 * seqs, 2 * seqs), jnp.float32)
    for r in range(0, tall, 2):
        x = jnp.concatenate([rows_of(r), rows_of(r + 1)], axis=1)
        total = total + dot(x, x, ((1,), (1,)))
    eye = lax.broadcasted_iota(jnp.int32, total.shape, 0) == lax.broadcasted_iota(
        jnp.int32, total.shape, 1
    )
    diag = jnp.sum(jnp.where(eye, total, 0.0), axis=0, keepdims=True)
    rows = jnp.concatenate([total, jnp.broadcast_to(diag, total.shape)], axis=1)
    copies = rows_out.shape[0] // rows.shape[0]
    for k in range(copies):
        rows_out[pl.ds(k, rows.shape[0], stride=copies), :] = rows


def final_body(at, got, out):
    seqs = out.shape[1]
    total = jnp.sum(got[...], axis=0, keepdims=True)
    lane = lax.broadcasted_iota(jnp.int32, total.shape, 1)
    own_diag = jnp.sum(jnp.where(lane == at[3] + seqs, total, 0.0), axis=1, keepdims=True)
    diag = pltpu.roll(total, seqs, 1)
    out[...] = (total / jnp.sqrt(own_diag * diag))[:, :seqs]


def on_device(states, cotangent, wq, wk, wv, wo):
    bf16, f32 = jnp.bfloat16, jnp.float32
    shape = jax.ShapeDtypeStruct
    length, part = states.shape[1:]
    states, cotangent = states[0], cotangent[0]
    axes = (lax.axis_index("h"), lax.axis_index("c"), lax.axis_index("zb"), lax.axis_index(SEQ))
    at = jnp.stack(axes).astype(jnp.int32)
    blocks = lax.axis_size(NEAR)
    seqs = 2 * blocks
    tall = (part + LANES) * (2 * part) // (LANES * blocks)

    def around(step):
        ring = (0, 2, 1, 3)
        return [(ring[q], ring[(q + step) % 4]) for q in range(4)]

    def moved(piece, step):
        return lax.ppermute(piece, ("zb", "h"), around(step))

    def near(piece):
        return piece, swapped(piece, "c")

    def gathered(own, relayed):
        up, down = moved(own, 1), moved(own, -1)
        far = moved(up if relayed == 1 else down, relayed)
        kinds = (own, far, up, down)
        return [part for piece in kinds for part in near(piece)]

    s_parts, c_parts = gathered(states, 1), gathered(cotangent, -1)
    cos, sine = rope_tables(length, HEAD_DIM)
    width = part // 2
    wq, wk, wv, wo = kernel_call(
        fetch_body,
        tuple(
            shape(dims, bf16)
            for dims in ((wq.shape[0], width), wk.shape, wv.shape, (width, wo.shape[1]))
        ),
        (at, wq, wk, wv, wo),
        (pltpu.SemaphoreType.DMA((4,)),),
        far=(1, 2, 3, 4),
    )

    def attention(partner, parts):
        return kernel_call(
            functools.partial(attention_body, partner),
            (
                shape((length, width), bf16),
                shape((width // HEAD_DIM * length, length), bf16),
            ),
            (at, *parts, wq, wk, wv, cos, sine),
        )

    partner_found = attention(True, s_parts[4:])
    own_found = attention(False, s_parts[:4])
    sent = kernel_call(
        blocks_body,
        shape((blocks, 2 * tall, LANES), bf16),
        (at, *s_parts, *c_parts, wo, *own_found, *partner_found),
    )
    got = lax.all_to_all(sent, NEAR, 0, 0, tiled=True)
    copies = lax.axis_size(TP)
    rows = kernel_call(
        share_body,
        shape((seqs * copies, 2 * seqs), f32),
        (at, got),
        (pltpu.VMEM((seqs * tall, LANES), f32),),
    )
    rows = rows.reshape(seqs * copies, 1, 2 * seqs)
    got = lax.all_to_all(rows, EVERY, 0, 0, tiled=True).reshape(seqs * copies, 2 * seqs)
    return kernel_call(final_body, shape((1, seqs), f32), (at, got))


def solution(mesh):
    split = Mesh(mesh.devices.reshape(2, mesh.shape["seq"] // 32, 4, 4, 2, 2), EVERY)
    placed = (
        P(SEQ, None, TP),
        P(SEQ, None, TP),
        P(None, TP),
        P(None, TP),
        P(None, TP),
        P(TP, None),
    )

    return jax.shard_map(
        on_device, mesh=split, in_specs=placed, out_specs=P(SEQ, None), check_vma=False
    )
```

```python
import functools

import functools

import jax
import jax.numpy as jnp
import numpy as np
from jax import lax
from jax.experimental import pallas as pl
from jax.experimental.pallas import tpu as pltpu
from jax.sharding import Mesh
from jax.sharding import PartitionSpec as P


HEAD_DIM = 64
LANES = 128
SEQ = ("zb", "za", "x", "y")
NEAR = ("za", "x", "y")
TP = ("h", "c")
EVERY = SEQ + TP
SWAP = ((0, 1), (1, 0))


theta_base = 500000.0


def swapped(value, axis):
    return lax.ppermute(value, axis, SWAP)


def rope_tables(length, head_dim):
    half_dim = head_dim // 2
    steps = np.arange(half_dim, dtype=np.float32) * np.float32(2.0) / np.float32(head_dim)
    freqs_k = np.power(np.float32(theta_base), -steps)
    angles = np.arange(length, dtype=np.float32)[:, None] * freqs_k[None, :]
    sine = np.sin(angles)
    cos = np.tile(np.cos(angles), (1, LANES // half_dim))
    return cos, np.tile(np.concatenate([-sine, sine], axis=1), (1, LANES // head_dim))


def dot(left, right, dims=((1,), (0,))):
    return lax.dot_general(left, right, (dims, ((), ())), preferred_element_type=jnp.float32)


def kernel_call(body, outs, ins, scratch=(), vmem_mib=20, far=()):
    ins = [pltpu.with_memory_space_constraint(a, pltpu.HBM) if i in far else a for i, a in enumerate(ins)]
    hbm = pl.BlockSpec(memory_space=pltpu.HBM)
    vmem = pl.BlockSpec(memory_space=pltpu.VMEM)

    def with_place(*refs):
        zb, za, x, y = (lax.axis_index(a) for a in SEQ)
        place = ((zb * lax.axis_size("za") + za) * lax.axis_size("x") + x) * lax.axis_size("y") + y
        body((lax.axis_index("h"), lax.axis_index("c"), zb, place), *refs)

    return pl.pallas_call(
        with_place,
        out_shape=outs,
        in_specs=[
            hbm if i in far else vmem for i in range(len(ins))
        ],
        out_specs=jax.tree.map(lambda _: vmem, outs),
        scratch_shapes=scratch,
        compiler_params=pltpu.CompilerParams(vmem_limit_bytes=vmem_mib * 2**20),
    )(*ins)


def lower_half(shape):
    return lax.broadcasted_iota(jnp.int32, shape, 1) % (2 * HEAD_DIM) < HEAD_DIM


def doubled(pair, low):
    turned = pltpu.roll(pair, HEAD_DIM, 1)
    return jnp.where(low, pair, turned), jnp.where(low, turned, pair)


def rows_at(place, size):
    return pl.ds(pl.multiple_of(place * size, size), size)


def places_of(at):
    h, c = at[0], at[1]
    return [2 * h + c, 2 * h + 1 - c, 2 * (1 - h) + c, 2 * (1 - h) + 1 - c]


def own_quarters(parts):
    return [part[...] for part in parts]


def partner_quarters(at, parts):
    straight = at[2] == 0
    values = [part[...] for part in parts]
    up, down = values[:2], values[2:]
    here = [jnp.where(straight, d, u) for u, d in zip(up, down)]
    return here + [jnp.where(straight, u, d) for u, d in zip(up, down)]


def fetch_body(at, wq, wk, wv, wo, wq_out, wk_out, wv_out, wo_out, sems):
    part = wq_out.shape[1]
    half = rows_at(at[2], part)
    moves = [
        pltpu.make_async_copy(src, dst, sems.at[i])
        for i, (src, dst) in enumerate(
            ((wq.at[:, half], wq_out), (wk, wk_out), (wv, wv_out), (wo.at[half, :], wo_out))
        )
    ]
    for move in moves:
        move.start()
    for move in moves:
        move.wait()


def attention_body(partner, at, *refs):
    *found, wq, wk, wv, cos_ref, sine_ref, attended, probs = refs
    parts = partner_quarters(at, found) if partner else own_quarters(found)
    quarter = parts[0].shape[1]

    def project(w):
        total = None
        for part, place in zip(parts, places_of(at)):
            term = dot(part, w[rows_at(place, quarter), :])
            total = term if total is None else total + term
        return total

    cos, sine = cos_ref[...], sine_ref[...]
    length = cos.shape[0]
    lane = lax.broadcasted_iota(jnp.int32, cos.shape, 1)
    first = lane % HEAD_DIM < HEAD_DIM // 2
    low = lower_half(cos.shape)
    straight = at[2] == 0

    def rotate(tile):
        ahead = pltpu.roll(tile, LANES - HEAD_DIM // 2, 1)
        behind = pltpu.roll(tile, HEAD_DIM // 2, 1)
        return tile * cos + jnp.where(first, ahead, behind) * sine

    def own_head(tile):
        even, odd = doubled(tile, low)
        return jnp.where(straight, even, odd).astype(jnp.bfloat16)

    keys, values, queries = own_head(rotate(project(wk))), own_head(project(wv)), project(wq)
    causal = lax.broadcasted_iota(jnp.int32, (length, length), 0) >= lax.broadcasted_iota(
        jnp.int32, (length, length), 1
    )
    for t in range(queries.shape[1] // LANES):
        query = rotate(queries[:, t * LANES : (t + 1) * LANES])
        found = []
        for s in range(2):
            mine = low if s == 0 else jnp.logical_not(low)
            q = jnp.where(mine, query, 0.0).astype(jnp.bfloat16)
            scores = dot(q, keys, ((1,), (1,))) * HEAD_DIM ** (-0.5)
            scores = jnp.where(causal, scores, -jnp.inf)
            e = jnp.exp(scores - jnp.max(scores, axis=1, keepdims=True))
            p = (e / jnp.sum(e, axis=1, keepdims=True)).astype(jnp.bfloat16)
            probs[(2 * t + s) * length : (2 * t + s + 1) * length, :] = p
            found.append(dot(p, values))
        tile = jnp.where(low, found[0], found[1])
        attended[:, t * LANES : (t + 1) * LANES] = tile.astype(jnp.bfloat16)


def blocks_body(at, *refs):
    s_refs, c_refs = refs[:8], refs[8:16]
    wo, attended_own, probs_own, attended_partner, probs_partner, blocks = refs[16:]
    attended, probs = (attended_own, attended_partner), (probs_own, probs_partner)
    states = list(zip(own_quarters(s_refs[:4]), partner_quarters(at, s_refs[4:])))
    cots = list(zip(own_quarters(c_refs[:4]), partner_quarters(at, c_refs[4:])))
    places = places_of(at)
    length, quarter = states[0][0].shape
    grads = None
    for pair, place in zip(cots, places):
        term = dot(jnp.concatenate(pair, axis=0), wo[:, rows_at(place, quarter)], ((1,), (1,)))
        grads = term if grads is None else grads + term
    low = lower_half((length, LANES))
    width = attended_own.shape[1]
    tiles = width // LANES
    tall = blocks.shape[1] // 2
    across = 4 * quarter // LANES
    for n in range(2):
        rows = slice(n * length, (n + 1) * length)
        stacked = []
        for t in range(tiles):
            tile = grads[rows, t * LANES : (t + 1) * LANES]
            stacked.append(jnp.where(low, tile, 0.0).astype(jnp.bfloat16))
            stacked.append(jnp.where(low, 0.0, tile).astype(jnp.bfloat16))
        found = dot(probs[n][...], jnp.concatenate(stacked, 0), ((0,), (0,)))
        value_gradient = (found + pltpu.roll(found, HEAD_DIM, 1)).astype(jnp.bfloat16)
        turned_a = attended[n][...].T
        turned_v = value_gradient.T[:HEAD_DIM, :]
        for k, place in enumerate(places):
            upper = dot(turned_a, cots[k][n]).astype(jnp.bfloat16)
            lower = dot(turned_v, states[k][n]).astype(jnp.bfloat16)
            for j in range(quarter // LANES):
                cols = slice(j * LANES, (j + 1) * LANES)
                at_col = place * (quarter // LANES) + j
                begin = n * tall
                blocks[at_col, begin : begin + tall, :] = upper[:tall, cols]
                rest = width - tall
                blocks[across + at_col, begin : begin + rest, :] = upper[tall:, cols]
                blocks[across + at_col, begin + rest : begin + tall, :] = lower[:, cols]


def share_body(at, got, rows_out, wide):
    seqs, both, _ = got.shape
    tall = both // 2
    straight = at[2] == 0
    for s in range(seqs):
        for t in range(both // 8):
            wide[pl.ds((t * seqs + s) * 8, 8), :] = got[s, t * 8 : t * 8 + 8, :].astype(jnp.float32)

    def rows_of(r):
        found = []
        for k in range(2):
            t, rest = divmod(r + k * tall, 8)
            rows = wide[pl.ds(t * seqs * 8 + rest, seqs, stride=8), :]
            found.append(rows.astype(jnp.bfloat16))
        return jnp.concatenate(
            [jnp.where(straight, found[0], found[1]), jnp.where(straight, found[1], found[0])], axis=0
        )

    total = jnp.zeros((2 * seqs, 2 * seqs), jnp.float32)
    for r in range(0, tall, 2):
        x = jnp.concatenate([rows_of(r), rows_of(r + 1)], axis=1)
        total = total + dot(x, x, ((1,), (1,)))
    eye = lax.broadcasted_iota(jnp.int32, total.shape, 0) == lax.broadcasted_iota(
        jnp.int32, total.shape, 1
    )
    diag = jnp.sum(jnp.where(eye, total, 0.0), axis=0, keepdims=True)
    rows = jnp.concatenate([total, jnp.broadcast_to(diag, total.shape)], axis=1)
    copies = rows_out.shape[0] // rows.shape[0]
    for k in range(copies):
        rows_out[pl.ds(k, rows.shape[0], stride=copies), :] = rows


def final_body(at, got, out):
    seqs = out.shape[1]
    total = jnp.sum(got[...], axis=0, keepdims=True)
    lane = lax.broadcasted_iota(jnp.int32, total.shape, 1)
    own_diag = jnp.sum(jnp.where(lane == at[3] + seqs, total, 0.0), axis=1, keepdims=True)
    diag = pltpu.roll(total, seqs, 1)
    out[...] = (total / jnp.sqrt(own_diag * diag))[:, :seqs]


def on_device(states, cotangent, wq, wk, wv, wo):
    bf16, f32 = jnp.bfloat16, jnp.float32
    shape = jax.ShapeDtypeStruct
    length, part = states.shape[1:]
    states, cotangent = states[0], cotangent[0]
    blocks = lax.axis_size(NEAR)
    seqs = 2 * blocks
    tall = (part + LANES) * (2 * part) // (LANES * blocks)

    def around(step):
        ring = (0, 2, 1, 3)
        return [(ring[q], ring[(q + step) % 4]) for q in range(4)]

    def moved(piece, step):
        return lax.ppermute(piece, ("zb", "h"), around(step))

    def near(piece):
        return piece, swapped(piece, "c")

    def gathered(own, relayed):
        up, down = moved(own, 1), moved(own, -1)
        far = moved(up if relayed == 1 else down, relayed)
        kinds = (own, far, up, down)
        return [part for piece in kinds for part in near(piece)]

    s_parts, c_parts = gathered(states, 1), gathered(cotangent, -1)
    cos, sine = rope_tables(length, HEAD_DIM)
    width = part // 2
    wq, wk, wv, wo = kernel_call(
        fetch_body,
        tuple(
            shape(dims, bf16)
            for dims in ((wq.shape[0], width), wk.shape, wv.shape, (width, wo.shape[1]))
        ),
        (wq, wk, wv, wo),
        (pltpu.SemaphoreType.DMA((4,)),),
        far=(0, 1, 2, 3),
    )

    def attention(partner, parts):
        return kernel_call(
            functools.partial(attention_body, partner),
            (
                shape((length, width), bf16),
                shape((width // HEAD_DIM * length, length), bf16),
            ),
            (*parts, wq, wk, wv, cos, sine),
        )

    partner_found = attention(True, s_parts[4:])
    own_found = attention(False, s_parts[:4])
    sent = kernel_call(
        blocks_body,
        shape((blocks, 2 * tall, LANES), bf16),
        (*s_parts, *c_parts, wo, *own_found, *partner_found),
    )
    got = lax.all_to_all(sent, NEAR, 0, 0, tiled=True)
    copies = lax.axis_size(TP)
    rows = kernel_call(
        share_body,
        shape((seqs * copies, 2 * seqs), f32),
        (got,),
        (pltpu.VMEM((seqs * tall, LANES), f32),),
    )
    rows = rows.reshape(seqs * copies, 1, 2 * seqs)
    got = lax.all_to_all(rows, EVERY, 0, 0, tiled=True).reshape(seqs * copies, 2 * seqs)
    return kernel_call(final_body, shape((1, seqs), f32), (got,))


def solution(mesh):
    split = Mesh(mesh.devices.reshape(2, mesh.shape["seq"] // 32, 4, 4, 2, 2), EVERY)
    placed = (
        P(SEQ, None, TP),
        P(SEQ, None, TP),
        P(None, TP),
        P(None, TP),
        P(None, TP),
        P(TP, None),
    )

    return jax.shard_map(
        on_device, mesh=split, in_specs=placed, out_specs=P(SEQ, None), check_vma=False
    )
```

```python
import functools

import functools

import jax
import jax.numpy as jnp
import numpy as np
from jax import lax
from jax.experimental import pallas as pl
from jax.experimental.pallas import tpu as pltpu
from jax.sharding import Mesh
from jax.sharding import PartitionSpec as P


HEAD_DIM = 64
LANES = 128
SEQ = ("zb", "za", "x", "y")
NEAR = ("za", "x", "y")
TP = ("h", "c")
EVERY = SEQ + TP
SWAP = ((0, 1), (1, 0))


theta_base = 500000.0


def swapped(value, axis):
    return lax.ppermute(value, axis, SWAP)


def rope_tables(length, head_dim):
    half_dim = head_dim // 2
    steps = np.arange(half_dim, dtype=np.float32) * np.float32(2.0) / np.float32(head_dim)
    freqs_k = np.power(np.float32(theta_base), -steps)
    angles = np.arange(length, dtype=np.float32)[:, None] * freqs_k[None, :]
    sine = np.sin(angles)
    cos = np.tile(np.cos(angles), (1, LANES // half_dim))
    return cos, np.tile(np.concatenate([-sine, sine], axis=1), (1, LANES // head_dim))


def dot(left, right, dims=((1,), (0,))):
    return lax.dot_general(left, right, (dims, ((), ())), preferred_element_type=jnp.float32)


def kernel_call(body, outs, ins, scratch=(), vmem_mib=20, far=()):
    ins = [pltpu.with_memory_space_constraint(a, pltpu.HBM) if i in far else a for i, a in enumerate(ins)]
    hbm = pl.BlockSpec(memory_space=pltpu.HBM)
    vmem = pl.BlockSpec(memory_space=pltpu.VMEM)

    def with_place(*refs):
        zb, za, x, y = (lax.axis_index(a) for a in SEQ)
        place = ((zb * lax.axis_size("za") + za) * lax.axis_size("x") + x) * lax.axis_size("y") + y
        body((lax.axis_index("h"), lax.axis_index("c"), zb, place), *refs)

    return pl.pallas_call(
        with_place,
        out_shape=outs,
        in_specs=[
            hbm if i in far else vmem for i in range(len(ins))
        ],
        out_specs=jax.tree.map(lambda _: vmem, outs),
        scratch_shapes=scratch,
        compiler_params=pltpu.CompilerParams(vmem_limit_bytes=vmem_mib * 2**20),
    )(*ins)


def lower_half(shape):
    return lax.broadcasted_iota(jnp.int32, shape, 1) % (2 * HEAD_DIM) < HEAD_DIM


def doubled(pair, low):
    turned = pltpu.roll(pair, HEAD_DIM, 1)
    return jnp.where(low, pair, turned), jnp.where(low, turned, pair)


def rows_at(place, size):
    return pl.ds(pl.multiple_of(place * size, size), size)


def places_of(at):
    h, c = at[0], at[1]
    return [2 * h + c, 2 * h + 1 - c, 2 * (1 - h) + c, 2 * (1 - h) + 1 - c]


def own_quarters(parts):
    values = [part[...] for part in parts]
    far = [jnp.concatenate([values[2 + k], values[4 + k]], axis=0) for k in range(2)]
    return values[:2] + far


def partner_quarters(at, parts):
    straight = at[2] == 0
    values = [part[...] for part in parts]
    up, down = values[:2], values[2:]
    here = [jnp.where(straight, d, u) for u, d in zip(up, down)]
    return here + [jnp.where(straight, u, d) for u, d in zip(up, down)]


def fetch_body(at, wq, wk, wv, wo, wq_out, wk_out, wv_out, wo_out, sems):
    part = wq_out.shape[1]
    half = rows_at(at[2], part)
    moves = [
        pltpu.make_async_copy(src, dst, sems.at[i])
        for i, (src, dst) in enumerate(
            ((wq.at[:, half], wq_out), (wk, wk_out), (wv, wv_out), (wo.at[half, :], wo_out))
        )
    ]
    for move in moves:
        move.start()
    for move in moves:
        move.wait()


def attention_body(partner, at, *refs):
    *found, wq, wk, wv, cos_ref, sine_ref, attended, probs = refs
    parts = partner_quarters(at, found) if partner else own_quarters(found)
    quarter = parts[0].shape[1]

    def project(w):
        total = None
        for part, place in zip(parts, places_of(at)):
            term = dot(part, w[rows_at(place, quarter), :])
            total = term if total is None else total + term
        return total

    cos, sine = cos_ref[...], sine_ref[...]
    length = cos.shape[0]
    lane = lax.broadcasted_iota(jnp.int32, cos.shape, 1)
    first = lane % HEAD_DIM < HEAD_DIM // 2
    low = lower_half(cos.shape)
    straight = at[2] == 0

    def rotate(tile):
        ahead = pltpu.roll(tile, LANES - HEAD_DIM // 2, 1)
        behind = pltpu.roll(tile, HEAD_DIM // 2, 1)
        return tile * cos + jnp.where(first, ahead, behind) * sine

    def own_head(tile):
        even, odd = doubled(tile, low)
        return jnp.where(straight, even, odd).astype(jnp.bfloat16)

    keys, values, queries = own_head(rotate(project(wk))), own_head(project(wv)), project(wq)
    causal = lax.broadcasted_iota(jnp.int32, (length, length), 0) >= lax.broadcasted_iota(
        jnp.int32, (length, length), 1
    )
    for t in range(queries.shape[1] // LANES):
        query = rotate(queries[:, t * LANES : (t + 1) * LANES])
        found = []
        for s in range(2):
            mine = low if s == 0 else jnp.logical_not(low)
            q = jnp.where(mine, query, 0.0).astype(jnp.bfloat16)
            scores = dot(q, keys, ((1,), (1,))) * HEAD_DIM ** (-0.5)
            scores = jnp.where(causal, scores, -jnp.inf)
            e = jnp.exp(scores - jnp.max(scores, axis=1, keepdims=True))
            p = (e / jnp.sum(e, axis=1, keepdims=True)).astype(jnp.bfloat16)
            probs[(2 * t + s) * length : (2 * t + s + 1) * length, :] = p
            found.append(dot(p, values))
        tile = jnp.where(low, found[0], found[1])
        attended[:, t * LANES : (t + 1) * LANES] = tile.astype(jnp.bfloat16)


def blocks_body(at, *refs):
    s_refs, c_refs = refs[:10], refs[10:20]
    wo, attended_own, probs_own, attended_partner, probs_partner, blocks = refs[20:]
    attended, probs = (attended_own, attended_partner), (probs_own, probs_partner)
    states = list(zip(own_quarters(s_refs[:6]), partner_quarters(at, s_refs[6:])))
    cots = list(zip(own_quarters(c_refs[:6]), partner_quarters(at, c_refs[6:])))
    places = places_of(at)
    length, quarter = states[0][0].shape
    grads = None
    for pair, place in zip(cots, places):
        term = dot(jnp.concatenate(pair, axis=0), wo[:, rows_at(place, quarter)], ((1,), (1,)))
        grads = term if grads is None else grads + term
    low = lower_half((length, LANES))
    width = attended_own.shape[1]
    tiles = width // LANES
    tall = blocks.shape[1] // 2
    across = 4 * quarter // LANES
    for n in range(2):
        rows = slice(n * length, (n + 1) * length)
        stacked = []
        for t in range(tiles):
            tile = grads[rows, t * LANES : (t + 1) * LANES]
            stacked.append(jnp.where(low, tile, 0.0).astype(jnp.bfloat16))
            stacked.append(jnp.where(low, 0.0, tile).astype(jnp.bfloat16))
        found = dot(probs[n][...], jnp.concatenate(stacked, 0), ((0,), (0,)))
        value_gradient = (found + pltpu.roll(found, HEAD_DIM, 1)).astype(jnp.bfloat16)
        turned_a = attended[n][...].T
        turned_v = value_gradient.T[:HEAD_DIM, :]
        for k, place in enumerate(places):
            upper = dot(turned_a, cots[k][n]).astype(jnp.bfloat16)
            lower = dot(turned_v, states[k][n]).astype(jnp.bfloat16)
            for j in range(quarter // LANES):
                cols = slice(j * LANES, (j + 1) * LANES)
                at_col = place * (quarter // LANES) + j
                begin = n * tall
                blocks[at_col, begin : begin + tall, :] = upper[:tall, cols]
                rest = width - tall
                blocks[across + at_col, begin : begin + rest, :] = upper[tall:, cols]
                blocks[across + at_col, begin + rest : begin + tall, :] = lower[:, cols]


def share_body(at, got, rows_out, wide):
    seqs, both, _ = got.shape
    tall = both // 2
    straight = at[2] == 0
    for s in range(seqs):
        for t in range(both // 8):
            wide[pl.ds((t * seqs + s) * 8, 8), :] = got[s, t * 8 : t * 8 + 8, :].astype(jnp.float32)

    def rows_of(r):
        found = []
        for k in range(2):
            t, rest = divmod(r + k * tall, 8)
            rows = wide[pl.ds(t * seqs * 8 + rest, seqs, stride=8), :]
            found.append(rows.astype(jnp.bfloat16))
        return jnp.concatenate(
            [jnp.where(straight, found[0], found[1]), jnp.where(straight, found[1], found[0])], axis=0
        )

    total = jnp.zeros((2 * seqs, 2 * seqs), jnp.float32)
    for r in range(0, tall, 2):
        x = jnp.concatenate([rows_of(r), rows_of(r + 1)], axis=1)
        total = total + dot(x, x, ((1,), (1,)))
    eye = lax.broadcasted_iota(jnp.int32, total.shape, 0) == lax.broadcasted_iota(
        jnp.int32, total.shape, 1
    )
    diag = jnp.sum(jnp.where(eye, total, 0.0), axis=0, keepdims=True)
    rows = jnp.concatenate([total, jnp.broadcast_to(diag, total.shape)], axis=1)
    copies = rows_out.shape[0] // rows.shape[0]
    for k in range(copies):
        rows_out[pl.ds(k, rows.shape[0], stride=copies), :] = rows


def final_body(at, got, out):
    seqs = out.shape[1]
    total = jnp.sum(got[...], axis=0, keepdims=True)
    lane = lax.broadcasted_iota(jnp.int32, total.shape, 1)
    own_diag = jnp.sum(jnp.where(lane == at[3] + seqs, total, 0.0), axis=1, keepdims=True)
    diag = pltpu.roll(total, seqs, 1)
    out[...] = (total / jnp.sqrt(own_diag * diag))[:, :seqs]


def on_device(states, cotangent, wq, wk, wv, wo):
    bf16, f32 = jnp.bfloat16, jnp.float32
    shape = jax.ShapeDtypeStruct
    length, part = states.shape[1:]
    states, cotangent = states[0], cotangent[0]
    blocks = lax.axis_size(NEAR)
    seqs = 2 * blocks
    tall = (part + LANES) * (2 * part) // (LANES * blocks)

    def around(step):
        ring = (0, 2, 1, 3)
        return [(ring[q], ring[(q + step) % 4]) for q in range(4)]

    def moved(piece, step):
        return lax.ppermute(piece, ("zb", "h"), around(step))

    def near(piece):
        return piece, swapped(piece, "c")

    def gathered(own):
        up, down = moved(own, 1), moved(own, -1)
        half = length // 2
        low, high = moved(up[:half], 1), moved(down[half:], -1)
        kinds = (own, low, high, up, down)
        return [part for piece in kinds for part in near(piece)]

    s_parts, c_parts = gathered(states), gathered(cotangent)
    cos, sine = rope_tables(length, HEAD_DIM)
    width = part // 2
    wq, wk, wv, wo = kernel_call(
        fetch_body,
        tuple(
            shape(dims, bf16)
            for dims in ((wq.shape[0], width), wk.shape, wv.shape, (width, wo.shape[1]))
        ),
        (wq, wk, wv, wo),
        (pltpu.SemaphoreType.DMA((4,)),),
        far=(0, 1, 2, 3),
    )

    def attention(partner, parts):
        return kernel_call(
            functools.partial(attention_body, partner),
            (
                shape((length, width), bf16),
                shape((width // HEAD_DIM * length, length), bf16),
            ),
            (*parts, wq, wk, wv, cos, sine),
        )

    partner_found = attention(True, s_parts[6:])
    own_found = attention(False, s_parts[:6])
    sent = kernel_call(
        blocks_body,
        shape((blocks, 2 * tall, LANES), bf16),
        (*s_parts, *c_parts, wo, *own_found, *partner_found),
    )
    got = lax.all_to_all(sent, NEAR, 0, 0, tiled=True)
    copies = lax.axis_size(TP)
    rows = kernel_call(
        share_body,
        shape((seqs * copies, 2 * seqs), f32),
        (got,),
        (pltpu.VMEM((seqs * tall, LANES), f32),),
    )
    rows = rows.reshape(seqs * copies, 1, 2 * seqs)
    got = lax.all_to_all(rows, EVERY, 0, 0, tiled=True).reshape(seqs * copies, 2 * seqs)
    return kernel_call(final_body, shape((1, seqs), f32), (got,))


def solution(mesh):
    split = Mesh(mesh.devices.reshape(2, mesh.shape["seq"] // 32, 4, 4, 2, 2), EVERY)
    placed = (
        P(SEQ, None, TP),
        P(SEQ, None, TP),
        P(None, TP),
        P(None, TP),
        P(None, TP),
        P(TP, None),
    )

    return jax.shard_map(
        on_device, mesh=split, in_specs=placed, out_specs=P(SEQ, None), check_vma=False
    )
```

```python
import functools

import functools

import jax
import jax.numpy as jnp
import numpy as np
from jax import lax
from jax.experimental import pallas as pl
from jax.experimental.pallas import tpu as pltpu
from jax.sharding import Mesh
from jax.sharding import PartitionSpec as P


HEAD_DIM = 64
LANES = 128
SEQ = ("zb", "za", "x", "y")
NEAR = ("za", "x", "y")
TP = ("h", "c")
EVERY = SEQ + TP
SWAP = ((0, 1), (1, 0))


theta_base = 500000.0


def swapped(value, axis):
    return lax.ppermute(value, axis, SWAP)


def rope_tables(length, head_dim):
    half_dim = head_dim // 2
    steps = np.arange(half_dim, dtype=np.float32) * np.float32(2.0) / np.float32(head_dim)
    freqs_k = np.power(np.float32(theta_base), -steps)
    angles = np.arange(length, dtype=np.float32)[:, None] * freqs_k[None, :]
    sine = np.sin(angles)
    cos = np.tile(np.cos(angles), (1, LANES // half_dim))
    return cos, np.tile(np.concatenate([-sine, sine], axis=1), (1, LANES // head_dim))


def dot(left, right, dims=((1,), (0,))):
    return lax.dot_general(left, right, (dims, ((), ())), preferred_element_type=jnp.float32)


def kernel_call(body, outs, ins, scratch=(), vmem_mib=20, far=()):
    ins = [pltpu.with_memory_space_constraint(a, pltpu.HBM) if i in far else a for i, a in enumerate(ins)]
    hbm = pl.BlockSpec(memory_space=pltpu.HBM)
    vmem = pl.BlockSpec(memory_space=pltpu.VMEM)

    def with_place(*refs):
        zb, za, x, y = (lax.axis_index(a) for a in SEQ)
        place = ((zb * lax.axis_size("za") + za) * lax.axis_size("x") + x) * lax.axis_size("y") + y
        body((lax.axis_index("h"), lax.axis_index("c"), zb, place), *refs)

    return pl.pallas_call(
        with_place,
        out_shape=outs,
        in_specs=[
            hbm if i in far else vmem for i in range(len(ins))
        ],
        out_specs=jax.tree.map(lambda _: vmem, outs),
        scratch_shapes=scratch,
        compiler_params=pltpu.CompilerParams(vmem_limit_bytes=vmem_mib * 2**20),
    )(*ins)


def lower_half(shape):
    return lax.broadcasted_iota(jnp.int32, shape, 1) % (2 * HEAD_DIM) < HEAD_DIM


def doubled(pair, low):
    turned = pltpu.roll(pair, HEAD_DIM, 1)
    return jnp.where(low, pair, turned), jnp.where(low, turned, pair)


def rows_at(place, size):
    return pl.ds(pl.multiple_of(place * size, size), size)


def places_of(at):
    h, c = at[0], at[1]
    return [2 * h + c, 2 * h + 1 - c, 2 * (1 - h) + c, 2 * (1 - h) + 1 - c]


def own_quarters(parts):
    return [part[...] for part in parts]


def partner_quarters(at, parts):
    straight = at[2] == 0
    values = [part[...] for part in parts]
    up, down = values[:2], values[2:]
    here = [jnp.where(straight, d, u) for u, d in zip(up, down)]
    return here + [jnp.where(straight, u, d) for u, d in zip(up, down)]


def attention_body(partner, at, *refs):
    *found, wq, wk, wv, cos_ref, sine_ref, attended, probs = refs
    parts = partner_quarters(at, found) if partner else own_quarters(found)
    quarter = parts[0].shape[1]

    def project(w):
        total = None
        for part, place in zip(parts, places_of(at)):
            term = dot(part, w[rows_at(place, quarter), :])
            total = term if total is None else total + term
        return total

    cos, sine = cos_ref[...], sine_ref[...]
    length = cos.shape[0]
    lane = lax.broadcasted_iota(jnp.int32, cos.shape, 1)
    first = lane % HEAD_DIM < HEAD_DIM // 2
    low = lower_half(cos.shape)
    straight = at[2] == 0

    def rotate(tile):
        ahead = pltpu.roll(tile, LANES - HEAD_DIM // 2, 1)
        behind = pltpu.roll(tile, HEAD_DIM // 2, 1)
        return tile * cos + jnp.where(first, ahead, behind) * sine

    def own_head(tile):
        even, odd = doubled(tile, low)
        return jnp.where(straight, even, odd).astype(jnp.bfloat16)

    keys, values, queries = own_head(rotate(project(wk))), own_head(project(wv)), project(wq)
    causal = lax.broadcasted_iota(jnp.int32, (length, length), 0) >= lax.broadcasted_iota(
        jnp.int32, (length, length), 1
    )
    for t in range(queries.shape[1] // LANES):
        query = rotate(queries[:, t * LANES : (t + 1) * LANES])
        found = []
        for s in range(2):
            mine = low if s == 0 else jnp.logical_not(low)
            q = jnp.where(mine, query, 0.0).astype(jnp.bfloat16)
            scores = dot(q, keys, ((1,), (1,))) * HEAD_DIM ** (-0.5)
            scores = jnp.where(causal, scores, -jnp.inf)
            e = jnp.exp(scores - jnp.max(scores, axis=1, keepdims=True))
            p = (e / jnp.sum(e, axis=1, keepdims=True)).astype(jnp.bfloat16)
            probs[(2 * t + s) * length : (2 * t + s + 1) * length, :] = p
            found.append(dot(p, values))
        tile = jnp.where(low, found[0], found[1])
        attended[:, t * LANES : (t + 1) * LANES] = tile.astype(jnp.bfloat16)


def first_attention_body(
    at, u0, u1, d0, d1, wq, wk, wv, cos, sine, wo,
    attended, probs, wq_out, wk_out, wv_out, cos_out, sine_out, wo_out, sems,
):
    half = rows_at(at[2], wq_out.shape[1])
    sources = (wq.at[:, half], wk, wv, cos, sine, wo.at[half, :])
    pairs = zip(sources, (wq_out, wk_out, wv_out, cos_out, sine_out, wo_out))
    moves = [pltpu.make_async_copy(src, dst, sems.at[i]) for i, (src, dst) in enumerate(pairs)]
    for move in moves:
        move.start()
    for move in moves[:5]:
        move.wait()
    attention_body(
        True, at, u0, u1, d0, d1, wq_out, wk_out, wv_out, cos_out, sine_out, attended, probs
    )
    moves[5].wait()


def blocks_body(at, *refs):
    s_refs, c_refs = refs[:8], refs[8:16]
    wo, attended_own, probs_own, attended_partner, probs_partner, blocks = refs[16:]
    attended, probs = (attended_own, attended_partner), (probs_own, probs_partner)
    states = list(zip(own_quarters(s_refs[:4]), partner_quarters(at, s_refs[4:])))
    cots = list(zip(own_quarters(c_refs[:4]), partner_quarters(at, c_refs[4:])))
    places = places_of(at)
    length, quarter = states[0][0].shape
    grads = None
    for pair, place in zip(cots, places):
        term = dot(jnp.concatenate(pair, axis=0), wo[:, rows_at(place, quarter)], ((1,), (1,)))
        grads = term if grads is None else grads + term
    low = lower_half((length, LANES))
    width = attended_own.shape[1]
    tiles = width // LANES
    tall = blocks.shape[1] // 2
    across = 4 * quarter // LANES
    for n in range(2):
        rows = slice(n * length, (n + 1) * length)
        stacked = []
        for t in range(tiles):
            tile = grads[rows, t * LANES : (t + 1) * LANES]
            stacked.append(jnp.where(low, tile, 0.0).astype(jnp.bfloat16))
            stacked.append(jnp.where(low, 0.0, tile).astype(jnp.bfloat16))
        found = dot(probs[n][...], jnp.concatenate(stacked, 0), ((0,), (0,)))
        value_gradient = (found + pltpu.roll(found, HEAD_DIM, 1)).astype(jnp.bfloat16)
        turned_a = attended[n][...].T
        turned_v = value_gradient.T[:HEAD_DIM, :]
        for k, place in enumerate(places):
            upper = dot(turned_a, cots[k][n]).astype(jnp.bfloat16)
            lower = dot(turned_v, states[k][n]).astype(jnp.bfloat16)
            for j in range(quarter // LANES):
                cols = slice(j * LANES, (j + 1) * LANES)
                at_col = place * (quarter // LANES) + j
                begin = n * tall
                blocks[at_col, begin : begin + tall, :] = upper[:tall, cols]
                rest = width - tall
                blocks[across + at_col, begin : begin + rest, :] = upper[tall:, cols]
                blocks[across + at_col, begin + rest : begin + tall, :] = lower[:, cols]


def share_body(at, got, rows_out, wide):
    seqs, both, _ = got.shape
    tall = both // 2
    straight = at[2] == 0
    for s in range(seqs):
        for t in range(both // 8):
            wide[pl.ds((t * seqs + s) * 8, 8), :] = got[s, t * 8 : t * 8 + 8, :].astype(jnp.float32)

    def rows_of(r):
        found = []
        for k in range(2):
            t, rest = divmod(r + k * tall, 8)
            rows = wide[pl.ds(t * seqs * 8 + rest, seqs, stride=8), :]
            found.append(rows.astype(jnp.bfloat16))
        return jnp.concatenate(
            [jnp.where(straight, found[0], found[1]), jnp.where(straight, found[1], found[0])], axis=0
        )

    total = jnp.zeros((2 * seqs, 2 * seqs), jnp.float32)
    for r in range(0, tall, 2):
        x = jnp.concatenate([rows_of(r), rows_of(r + 1)], axis=1)
        total = total + dot(x, x, ((1,), (1,)))
    eye = lax.broadcasted_iota(jnp.int32, total.shape, 0) == lax.broadcasted_iota(
        jnp.int32, total.shape, 1
    )
    diag = jnp.sum(jnp.where(eye, total, 0.0), axis=0, keepdims=True)
    rows = jnp.concatenate([total, jnp.broadcast_to(diag, total.shape)], axis=1)
    copies = rows_out.shape[0] // rows.shape[0]
    for k in range(copies):
        rows_out[pl.ds(k, rows.shape[0], stride=copies), :] = rows


def final_body(at, got, out):
    seqs = out.shape[1]
    total = jnp.sum(got[...], axis=0, keepdims=True)
    lane = lax.broadcasted_iota(jnp.int32, total.shape, 1)
    own_diag = jnp.sum(jnp.where(lane == at[3] + seqs, total, 0.0), axis=1, keepdims=True)
    diag = pltpu.roll(total, seqs, 1)
    out[...] = (total / jnp.sqrt(own_diag * diag))[:, :seqs]


def on_device(states, cotangent, wq, wk, wv, wo):
    bf16, f32 = jnp.bfloat16, jnp.float32
    shape = jax.ShapeDtypeStruct
    length, part = states.shape[1:]
    states, cotangent = states[0], cotangent[0]
    blocks = lax.axis_size(NEAR)
    seqs = 2 * blocks
    tall = (part + LANES) * (2 * part) // (LANES * blocks)

    def around(step):
        ring = (0, 2, 1, 3)
        return [(ring[q], ring[(q + step) % 4]) for q in range(4)]

    def moved(piece, step):
        return lax.ppermute(piece, ("zb", "h"), around(step))

    def near(piece):
        return piece, swapped(piece, "c")

    def gathered(own, relayed):
        up, down = moved(own, 1), moved(own, -1)
        far = moved(up if relayed == 1 else down, relayed)
        kinds = (own, far, up, down)
        return [part for piece in kinds for part in near(piece)]

    s_parts, c_parts = gathered(states, 1), gathered(cotangent, -1)
    cos, sine = rope_tables(length, HEAD_DIM)
    width = part // 2
    found = (shape((length, width), bf16), shape((width // HEAD_DIM * length, length), bf16))
    weights = ((wq.shape[0], width), wk.shape, wv.shape, (width, wo.shape[1]))
    *partner_found, wq, wk, wv, cos, sine, wo = kernel_call(
        first_attention_body,
        (
            *found,
            *(shape(dims, bf16) for dims in weights[:3]),
            *(shape(a.shape, f32) for a in (cos, sine)),
            shape(weights[3], bf16),
        ),
        (*s_parts[4:], wq, wk, wv, jnp.asarray(cos), jnp.asarray(sine), wo),
        (pltpu.SemaphoreType.DMA((6,)),),
        far=(4, 5, 6, 7, 8, 9),
    )
    own_found = kernel_call(
        functools.partial(attention_body, False),
        found,
        (*s_parts[:4], wq, wk, wv, cos, sine),
    )
    sent = kernel_call(
        blocks_body,
        shape((blocks, 2 * tall, LANES), bf16),
        (*s_parts, *c_parts, wo, *own_found, *partner_found),
    )
    got = lax.all_to_all(sent, NEAR, 0, 0, tiled=True)
    copies = lax.axis_size(TP)
    rows = kernel_call(
        share_body,
        shape((seqs * copies, 2 * seqs), f32),
        (got,),
        (pltpu.VMEM((seqs * tall, LANES), f32),),
    )
    rows = rows.reshape(seqs * copies, 1, 2 * seqs)
    got = lax.all_to_all(rows, EVERY, 0, 0, tiled=True).reshape(seqs * copies, 2 * seqs)
    return kernel_call(final_body, shape((1, seqs), f32), (got,))


def solution(mesh):
    split = Mesh(mesh.devices.reshape(2, mesh.shape["seq"] // 32, 4, 4, 2, 2), EVERY)
    placed = (
        P(SEQ, None, TP),
        P(SEQ, None, TP),
        P(None, TP),
        P(None, TP),
        P(None, TP),
        P(TP, None),
    )

    return jax.shard_map(
        on_device, mesh=split, in_specs=placed, out_specs=P(SEQ, None), check_vma=False
    )
```
